128 devices in a mesh: groups: 4 (over x, y), samp: 32 (over z, core).
Axes of the slice: x: 2, y: 2, z: 16, core: 2. Of those that a mesh axis runs over, the one named last changes fastest.
The devices are a block of a 8x8x16 slice.
Arguments:
- dosage: bfloat16 [32768, 8192], P(('groups', 'samp')), parts along dimension 0, may hold values from 0 to 2
- covariates: bfloat16 [32768, 96], P(('groups', 'samp')), parts along dimension 0, may hold values from -8 to 8
- expression: bfloat16 [32768, 16384], P('groups', 'samp'), parts along dimension 0, may hold values from -10 to 10
- block_index: int32 [8, 1024], P('groups'), parts along dimension 0, may hold values from 0 to 8191
- expr_row: int32 [32768], P('groups'), parts along dimension 0, may hold values from 0 to 8191, each once
Outputs:
- zscore: float32 [8192, 16384], P('groups', 'samp'), parts along dimension 0
The draws below stay inside these ranges and needn't reach their ends.
There are 4 independent parts, one for each index of `groups`. The reference program is written for one: setup_inputs(seed, part) draws one part's arguments, and reference() takes and returns one part's arrays. A program takes and returns all parts, laid end to end along the dimension named above; each array names one. Nothing has to cross between parts.
Inputs may be any that keep to these rules, and one draw needn't show every extreme that they name: `expr_row`: every expression row appears once.
All inputs are finite; a program needn't handle non-finite values.
Results may differ from the reference program's by a relative error of at most 0.0029.
Values may be sent and summed in bfloat16 or wider, within the bound.
No kernel may reach another device: no remote copies, remote signals or barrier semaphores. Data moves between devices by JAX's collectives and lax.ppermute only.
A program may use at most 192 MiB of HBM per device.

```python
import math
import jax
import jax.numpy as jnp
from jax import lax

K = 96
V = 1024
BLOCKS = 2
VPANEL = 8192
NSAMP = 8192
GENES = 16384


def covariate_base(key):
    first = jax.random.fold_in(key, 11)
    normal_part = jax.random.normal(first, (NSAMP, K), jnp.float32)
    rising = 1.0 + 2.0 * jnp.arange(NSAMP, dtype=jnp.float32) / NSAMP
    return jnp.clip(normal_part * rising[:, None], -8.0, 8.0)


def draw_covariates(key, part):
    return covariate_base(key).astype(jnp.bfloat16)


def draw_dosage(key, part):
    base = covariate_base(key)
    loading = jax.random.normal(jax.random.fold_in(key, 21), (K, VPANEL), jnp.float32)
    noise_key = jax.random.fold_in(key, 22)
    noise = jax.random.uniform(noise_key, (NSAMP, VPANEL), jnp.float32, -0.6, 0.6)
    shared = jnp.dot(base, loading) * (0.3 / K ** 0.5)
    return jnp.clip(1.0 + shared + noise, 0.0, 2.0).astype(jnp.bfloat16)


def draw_expression(key, part):
    base = covariate_base(key)
    loading = jax.random.normal(jax.random.fold_in(key, 31), (K, GENES), jnp.float32)
    noise_key = jax.random.fold_in(key, 32)
    noise = jax.random.normal(noise_key, (NSAMP, GENES), jnp.float32)
    shared = jnp.dot(base, loading) * (0.5 / K ** 0.5)
    return jnp.clip(shared + noise, -10.0, 10.0).astype(jnp.bfloat16)


def plant(entries, own_key, least, high):
    place = [jax.random.randint(jax.random.fold_in(own_key, axis), (), 0, length) for axis, length in enumerate(entries.shape)]
    widest = entries.shape.index(max(entries.shape))
    beside = place[:widest] + [(place[widest] + 1) % entries.shape[widest]] + place[widest + 1:]
    return entries.at[tuple(place)].set(least).at[tuple(beside)].set(high)


def setup_inputs(seed: int = 0, part: int = 0) -> dict:
    key_list = jax.random.split(jax.random.key(seed), 6)
    part_keys = jax.random.split(jax.random.fold_in(key_list[5], part), 6)
    dosage = draw_dosage(jax.random.fold_in(jax.random.fold_in(key_list[5], part), 71), part)
    covariates = draw_covariates(jax.random.fold_in(jax.random.fold_in(key_list[5], part), 71), part)
    expression = draw_expression(jax.random.fold_in(jax.random.fold_in(key_list[5], part), 71), part)
    block_index = plant(jax.random.randint(part_keys[3], (BLOCKS, V), 0, VPANEL), jax.random.fold_in(part_keys[3], 1), 0, VPANEL - 1).astype(jnp.int32)
    expr_row = jax.random.permutation(part_keys[4], NSAMP).astype(jnp.int32)
    return dict(dosage=dosage, covariates=covariates, expression=expression, block_index=block_index, expr_row=expr_row)


epsilon = 1e-06

def reference(dosage, covariates, expression, block_index, expr_row):
    gram = jnp.dot(covariates.T.astype(jnp.float32), covariates.astype(jnp.float32), preferred_element_type=jnp.float32)
    factor = jnp.linalg.cholesky(gram)
    matched = jnp.take(expression, expr_row, axis=0)
    panel_norm = lax.optimization_barrier(jnp.sum(jnp.square(expression.astype(jnp.float32)), axis=0))
    cov_float = covariates.astype(jnp.float32)
    scale = math.sqrt(NSAMP - K - 1)
    results = []
    for block in range(BLOCKS):
        picked = jnp.take(dosage, block_index[block], axis=1)
        loads = jnp.dot(covariates.T.astype(jnp.float32), picked.astype(jnp.float32), preferred_element_type=jnp.float32)
        coeffs = jax.scipy.linalg.cho_solve((factor, True), loads)
        fitted = jnp.dot(cov_float, coeffs, precision=lax.Precision.HIGHEST)
        resid = (picked.astype(jnp.float32) - fitted).astype(jnp.bfloat16)
        resid_norm = lax.optimization_barrier(jnp.sum(jnp.square(resid.astype(jnp.float32)), axis=0))
        products = jnp.dot(resid.T.astype(jnp.float32), matched.astype(jnp.float32), preferred_element_type=jnp.float32)
        results.append(scale * products * lax.rsqrt(resid_norm + epsilon)[:, None] * lax.rsqrt(panel_norm + epsilon)[None, :])
    return jnp.concatenate(results, axis=0)
```

```python
import math

import jax
import jax.numpy as jnp
from jax import lax
from jax.experimental import pallas as pl
from jax.experimental.pallas import tpu as pltpu
from jax.sharding import Mesh
from jax.sharding import PartitionSpec as P


GROUPS_SAMP = ("groups", "samp_0", "samp_1")
SAMP = ("samp_0", "samp_1")
LANES = 128
TILE = 256

epsilon = 1e-06


def pick_columns(dosage, block_index, block):
    samples, panel = dosage.shape
    blocks, width = block_index.shape
    tile = 512

    def kernel(index_ref, dosage_ref, out_ref, hot_ref):
        lane = lax.broadcasted_iota(jnp.int32, (LANES, LANES), 1)
        for part in range(tile // LANES):
            row = index_ref[block : block + 1, part * LANES : (part + 1) * LANES].astype(jnp.float32)
            column = jnp.broadcast_to(row, (LANES, LANES)).T.astype(jnp.int32) - lane
            for step in range(panel // LANES):
                hot = jnp.where(column == step * LANES, 1.0, 0.0).astype(jnp.bfloat16)
                hot_ref[pl.ds(part * LANES, LANES), pl.ds(step * LANES, LANES)] = hot
        out_ref[...] = lax.dot_general(
            hot_ref[...], dosage_ref[...], (((1,), (1,)), ((), ())), preferred_element_type=jnp.float32
        ).astype(jnp.bfloat16)

    return pl.pallas_call(
        kernel,
        out_shape=jax.ShapeDtypeStruct((width, samples), jnp.bfloat16),
        grid=(width // tile,),
        in_specs=[
            pl.BlockSpec((blocks, tile), lambda i: (0, i)),
            pl.BlockSpec((samples, panel), lambda i: (0, 0)),
        ],
        out_specs=pl.BlockSpec((tile, samples), lambda i: (i, 0)),
        scratch_shapes=[pltpu.VMEM((tile, panel), jnp.bfloat16)],
        cost_estimate=pl.CostEstimate(flops=2 * width * samples * panel, bytes_accessed=2 * samples * panel, transcendentals=0),
        compiler_params=pltpu.CompilerParams(vmem_limit_bytes=32 * 2**20),
        name="pick",
    )(block_index, dosage)


def match_rows(expression, expr_row, block_map, block):
    rows, genes = expression.shape
    parts = genes // LANES
    chunk = 128
    take = 4 * block

    def kernel(map_ref, row_ref, exp_ref, out_ref, norm_ref, wide_ref, got_ref):
        here = pl.program_id(0)

        @pl.when(here == 0)
        def _():
            def widen(step, sums):
                at = pl.multiple_of(step * chunk, chunk)
                value = exp_ref[pl.ds(at, chunk), :].astype(jnp.float32)
                for part in range(parts):
                    wide_ref[pl.ds(at * parts + part, chunk, stride=parts), :] = value[:, part * LANES : (part + 1) * LANES]
                square = value * value
                return sums + jnp.sum(square.reshape(chunk // 8, 8, genes), axis=0)

            sums = lax.fori_loop(0, rows // chunk, widen, jnp.zeros((8, genes), jnp.float32))
            norm_ref[...] = jnp.sum(sums, axis=0, keepdims=True)

        unroll = 64

        def fetch(step, carry):
            at = step * unroll
            base = map_ref[here * (take // block) + at // block] * block - (at // block) * block
            for k in range(unroll):
                source = pl.multiple_of(row_ref[base + at + k] * parts, parts)
                target = pl.multiple_of((at + k) * parts, parts)
                got_ref[pl.ds(target, parts), :] = wide_ref[pl.ds(source, parts), :]
            return carry

        lax.fori_loop(0, take // unroll, fetch, 0)
        for part in range(parts):
            out_ref[:, part * LANES : (part + 1) * LANES] = got_ref[pl.ds(part, take, stride=parts), :].astype(jnp.bfloat16)

    return pl.pallas_call(
        kernel,
        out_shape=(
            jax.ShapeDtypeStruct((rows, genes), jnp.bfloat16),
            jax.ShapeDtypeStruct((1, genes), jnp.float32),
        ),
        grid_spec=pltpu.PrefetchScalarGridSpec(
            num_scalar_prefetch=2,
            grid=(rows // take,),
            in_specs=[pl.BlockSpec((rows, genes), lambda i, m, r: (0, 0), pipeline_mode=pl.Buffered(1))],
            out_specs=[
                pl.BlockSpec((take, genes), lambda i, m, r: (i, 0)),
                pl.BlockSpec((1, genes), lambda i, m, r: (0, 0)),
            ],
            scratch_shapes=[
                pltpu.VMEM((rows * parts, LANES), jnp.float32),
                pltpu.VMEM((take * parts, LANES), jnp.float32),
            ],
        ),
        cost_estimate=pl.CostEstimate(flops=12 * 10**9, bytes_accessed=4 * rows * genes, transcendentals=0),
        compiler_params=pltpu.CompilerParams(vmem_limit_bytes=44 * 2**20),
        name="match",
    )(block_map, expr_row, expression)


def square_lanes(value):
    wide = value.astype(jnp.float32)
    wide = wide * wide
    total = wide[:, :LANES]
    for part in range(1, wide.shape[1] // LANES):
        total = total + wide[:, part * LANES : (part + 1) * LANES]
    return total


def dot(x, y):
    return jnp.dot(x, y, preferred_element_type=jnp.float32)


def fold_in(pieces, covars, matched, slots, state):
    count = len(pieces)
    width, samples = pieces[0].shape
    genes = matched.shape[1]
    covs = covars[0].shape[1]
    tile = 512
    first = state is None
    rows = count * samples // len(slots)

    def kernel(*refs):
        piece_refs = refs[:count]
        covar_refs = refs[count : 2 * count]
        matched_refs = refs[2 * count : 2 * count + len(slots)]
        rest = refs[2 * count + len(slots) :]
        outs = rest[-3:]
        whole = jnp.concatenate([ref[...] for ref in piece_refs], axis=1)
        cov = jnp.concatenate([ref[...] for ref in covar_refs], axis=0)
        sums = dot(whole, jnp.concatenate([ref[...] for ref in matched_refs], axis=0))
        loads = dot(whole, cov)
        norms = square_lanes(whole)
        if not first:
            sums = sums + rest[0][...]
            loads = loads + rest[1][...]
            norms = norms + rest[2][...]
        outs[0][...] = sums
        outs[1][...] = loads
        outs[2][...] = norms

    piece_spec = pl.BlockSpec((tile, samples), lambda i: (i, 0))
    covar_spec = pl.BlockSpec((samples, covs), lambda i: (0, 0))
    matched_specs = [pl.BlockSpec((rows, genes), lambda i, slot=slot: (slot, 0)) for slot in slots]
    state_specs = [
        pl.BlockSpec((tile, genes), lambda i: (i, 0)),
        pl.BlockSpec((tile, covs), lambda i: (i, 0)),
        pl.BlockSpec((tile, LANES), lambda i: (i, 0)),
    ]
    shapes = (
        jax.ShapeDtypeStruct((width, genes), jnp.float32),
        jax.ShapeDtypeStruct((width, covs), jnp.float32),
        jax.ShapeDtypeStruct((width, LANES), jnp.float32),
    )
    operands = [*pieces, *covars, *([matched] * len(slots)), *(() if first else state)]
    return pl.pallas_call(
        kernel,
        out_shape=shapes,
        grid=(width // tile,),
        in_specs=[piece_spec] * count + [covar_spec] * count + matched_specs + ([] if first else state_specs),
        out_specs=state_specs,
        input_output_aliases={} if first else {2 * count + len(slots) + k: k for k in range(3)},
        cost_estimate=pl.CostEstimate(
            flops=2 * width * samples * count * (genes + covs), bytes_accessed=8 * width * genes, transcendentals=0
        ),
        compiler_params=pltpu.CompilerParams(vmem_limit_bytes=24 * 2**20),
        name="fold",
    )(*operands)


def finish(low, high, covars, matched, group, state, inverse, loading, panel_norm, scale, out, half, halves):
    count = len(low)
    samples = low[0].shape[1]
    genes = matched.shape[1]
    covs = covars[0].shape[1]
    width = state[0].shape[0]
    tile = TILE
    steps = width // tile
    split = low[0].shape[0] // tile
    highest = lax.Precision.HIGHEST

    def kernel(*refs):
        low_refs = refs[:count]
        high_refs = refs[count : 2 * count]
        covar_refs = refs[2 * count : 3 * count]
        matched_ref, sum_ref, load_ref, square_ref, inverse_ref, loading_ref, panel_ref = refs[3 * count : 3 * count + 7]
        out_ref = refs[-1]

        def work(piece_refs):
            whole = jnp.concatenate([ref[...] for ref in piece_refs], axis=1)
            cov = jnp.concatenate([ref[...] for ref in covar_refs], axis=0)
            sums = sum_ref[...] + dot(whole, matched_ref[...])
            loads = load_ref[...] + dot(whole, cov)
            squares = jnp.sum(square_ref[...] + square_lanes(whole), axis=1, keepdims=True)
            white = jnp.dot(loads, inverse_ref[...], precision=highest)
            fitted = jnp.dot(white, loading_ref[...], precision=highest)
            resid_norm = jnp.maximum(squares - jnp.sum(white * white, axis=1, keepdims=True), 0.0)
            out_ref[...] = (
                scale * (sums - fitted) * lax.rsqrt(resid_norm + epsilon) * lax.rsqrt(panel_ref[...] + epsilon)
            )

        here = pl.program_id(0)

        @pl.when(here < split)
        def _():
            work(low_refs)

        @pl.when(here >= split)
        def _():
            work(high_refs)

    operands = [*low, *high, *covars, matched, *state, inverse, loading, panel_norm]
    in_specs = (
        [pl.BlockSpec((tile, samples), lambda i: (jnp.minimum(i, split - 1), 0))] * count
        + [pl.BlockSpec((tile, samples), lambda i: (jnp.maximum(i - split, 0), 0))] * count
        + [pl.BlockSpec((samples, covs), lambda i: (0, 0))] * count
        + [
            pl.BlockSpec((count * samples, genes), lambda i: (group, 0)),
            pl.BlockSpec((tile, genes), lambda i: (i, 0)),
            pl.BlockSpec((tile, covs), lambda i: (i, 0)),
            pl.BlockSpec((tile, LANES), lambda i: (i, 0)),
            pl.BlockSpec((covs, covs), lambda i: (0, 0)),
            pl.BlockSpec((covs, genes), lambda i: (0, 0)),
            pl.BlockSpec((1, genes), lambda i: (0, 0)),
        ]
    )
    aliases = {}
    if out is not None:
        aliases = {len(operands): 0}
        operands.append(out)
        in_specs.append(pl.BlockSpec(memory_space=pl.ANY))
    return pl.pallas_call(
        kernel,
        out_shape=jax.ShapeDtypeStruct((halves * width, genes), jnp.float32),
        grid=(steps,),
        in_specs=in_specs,
        out_specs=pl.BlockSpec((tile, genes), lambda i: (half * steps + i, 0)),
        input_output_aliases=aliases,
        cost_estimate=pl.CostEstimate(
            flops=2 * width * samples * count * genes + 14 * width * covs * genes,
            bytes_accessed=8 * width * genes,
            transcendentals=0,
        ),
        name="finish",
    )(*operands)


def whole(dosage, covariates, expression, block_index, expr_row):
    blocks = block_index.shape[0]
    covars = covariates.shape[1]
    here = dosage.shape[0]
    ring = lax.axis_size("samp_0")
    turns = ring // 2
    chip = lax.axis_index("samp_0")
    core = lax.axis_index("samp_1")
    scale = math.sqrt(expr_row.shape[0] - covars - 1)
    up = [(i, (i + 1) % ring) for i in range(ring)]
    down = [(i, (i - 1) % ring) for i in range(ring)]
    cross = [(0, 1), (1, 0)]

    def swap(x):
        return lax.ppermute(x, "samp_1", cross)

    order = [chip]
    for turn in range(1, turns):
        order += [chip - turn, chip + turn]
    order += [chip + turns]
    order = [chip_at % ring for chip_at in order]
    block_map = jnp.stack([2 * chip_at + side for chip_at in order for side in (core, 1 - core)]).astype(jnp.int32)

    flow = [None] * blocks
    covs = {}

    def pair_of(up_value, down_value):
        return (up_value, swap(up_value), down_value, swap(down_value))

    own = []
    for block in range(blocks):
        piece = pick_columns(dosage, block_index, block)
        own.append(piece)
        flow[block] = (piece, piece)
    cov_flow = (covariates, covariates)
    matched, panel_norm = match_rows(expression, expr_row, block_map, here)

    def shift(values, turn):
        up_value, down_value = values
        if turn == turns:
            middle = up_value.shape[0] // 2
            up_value, down_value = up_value[:middle], down_value[middle:]
        up_value = lax.ppermute(up_value, "samp_0", up)
        down_value = lax.ppermute(down_value, "samp_0", down)
        return up_value, down_value

    for turn in range(1, turns + 1):
        cov_flow = shift(cov_flow, turn)
        covs[turn] = cov_flow
    cov_pairs = {0: (covariates, swap(covariates))}
    for turn in range(1, turns):
        cov_pairs[turn] = pair_of(*covs[turn])
    last = jnp.concatenate(covs[turns], axis=0)
    cov_pairs[turns] = (last, swap(last))

    state = [None] * blocks
    arrived = [{0: (own[block], swap(own[block]))} for block in range(blocks)]

    def gather(turns_here, block):
        slots = []
        pieces = []
        covars_here = []
        for turn in turns_here:
            slots += [0] if turn == 0 else [2 * turn - 1, 2 * turn]
            pieces += arrived[block][turn]
            covars_here += cov_pairs[turn]
        return tuple(pieces), tuple(covars_here), matched, tuple(slots)

    for turn in range(1, turns):
        for block in range(blocks):
            flow[block] = shift(flow[block], turn)
            arrived[block][turn] = pair_of(*flow[block])
            if turn % 2 == 1:
                state[block] = fold_in(*gather((turn - 1, turn), block), state[block])

    every_cov = jnp.concatenate([piece for turn in range(turns + 1) for piece in cov_pairs[turn]], axis=0)
    gram = jnp.dot(every_cov.T, every_cov, preferred_element_type=jnp.float32)
    cross_loads = jnp.dot(every_cov.T, matched, preferred_element_type=jnp.float32)
    factor = jnp.linalg.cholesky(gram)
    inverse = lax.linalg.triangular_solve(factor, jnp.eye(covars, dtype=jnp.float32), left_side=True, lower=True)
    loading = jnp.dot(inverse, cross_loads, precision=lax.Precision.HIGHEST)

    out = None
    for block in range(blocks):
        flow[block] = shift(flow[block], turns)
        low, low_swap, high, high_swap = pair_of(*flow[block])
        out = finish(
            (low, low_swap),
            (high, high_swap),
            cov_pairs[turns],
            matched,
            ring - 1,
            state[block],
            inverse.T,
            loading,
            panel_norm,
            scale,
            out,
            block,
            blocks,
        )
    return out


def solution(mesh):
    torus = Mesh(mesh.devices.reshape(mesh.shape["groups"], -1, 2), ("groups", "samp_0", "samp_1"))
    in_specs = (
        P(GROUPS_SAMP, None),
        P(GROUPS_SAMP, None),
        P("groups", SAMP),
        P("groups", None),
        P("groups"),
    )
    out_specs = P("groups", SAMP)
    return jax.shard_map(whole, mesh=torus, in_specs=in_specs, out_specs=out_specs, check_vma=False)
```

```python
import math

import jax
import jax.numpy as jnp
from jax import lax
from jax.experimental import pallas as pl
from jax.experimental.pallas import tpu as pltpu
from jax.sharding import Mesh
from jax.sharding import PartitionSpec as P


GROUPS_SAMP = ("groups", "samp_0", "samp_1")
SAMP = ("samp_0", "samp_1")
LANES = 128

epsilon = 1e-06


def pick_columns(dosage, block_index, block, riders):
    samples, panel = dosage.shape
    blocks, width = block_index.shape
    tile = 512
    extra = riders[0].shape[0] if riders else 0
    copies = max(1, len(riders))

    def kernel(index_ref, dosage_ref, *refs):
        hot_ref = refs[-1]
        outs = refs[len(riders) : -1]
        here = pl.program_id(0)
        lane = lax.broadcasted_iota(jnp.int32, (LANES, LANES), 1)
        for part in range(tile // LANES):
            row = index_ref[block : block + 1, part * LANES : (part + 1) * LANES].astype(jnp.float32)
            column = jnp.broadcast_to(row, (LANES, LANES)).T.astype(jnp.int32) - lane
            for step in range(panel // LANES):
                hot = jnp.where(column == step * LANES, 1.0, 0.0).astype(jnp.bfloat16)
                hot_ref[pl.ds(part * LANES, LANES), pl.ds(step * LANES, LANES)] = hot
        picked = lax.dot_general(
            hot_ref[...], dosage_ref[...], (((1,), (1,)), ((), ())), preferred_element_type=jnp.float32
        ).astype(jnp.bfloat16)
        for out_ref in outs:
            out_ref[pl.ds(pl.multiple_of(here * tile, tile), tile), :] = picked
        for rider_ref, out_ref in zip(refs[: len(riders)], outs):
            out_ref[width:, :] = rider_ref[...]

    return pl.pallas_call(
        kernel,
        out_shape=(jax.ShapeDtypeStruct((width + extra, samples), jnp.bfloat16),) * copies,
        grid=(width // tile,),
        in_specs=[
            pl.BlockSpec((blocks, tile), lambda i: (0, i)),
            pl.BlockSpec((samples, panel), lambda i: (0, 0)),
        ]
        + [pl.BlockSpec((extra, samples), lambda i: (0, 0))] * len(riders),
        out_specs=(pl.BlockSpec((width + extra, samples), lambda i: (0, 0)),) * copies,
        scratch_shapes=[pltpu.VMEM((tile, panel), jnp.bfloat16)],
        cost_estimate=pl.CostEstimate(flops=2 * width * samples * panel, bytes_accessed=2 * samples * panel, transcendentals=0),
        compiler_params=pltpu.CompilerParams(vmem_limit_bytes=24 * 2**20),
        name="pick",
    )(block_index, dosage, *riders)


def match_rows(expression, expr_row, block_map, block):
    rows, genes = expression.shape
    parts = genes // LANES
    chunk = 128
    take = 4 * block

    def kernel(map_ref, row_ref, exp_ref, out_ref, norm_ref, wide_ref, got_ref):
        here = pl.program_id(0)

        @pl.when(here == 0)
        def _():
            def widen(step, sums):
                at = pl.multiple_of(step * chunk, chunk)
                value = exp_ref[pl.ds(at, chunk), :].astype(jnp.float32)
                for part in range(parts):
                    wide_ref[pl.ds(at * parts + part, chunk, stride=parts), :] = value[:, part * LANES : (part + 1) * LANES]
                square = value * value
                return sums + jnp.sum(square.reshape(chunk // 8, 8, genes), axis=0)

            sums = lax.fori_loop(0, rows // chunk, widen, jnp.zeros((8, genes), jnp.float32))
            norm_ref[...] = jnp.sum(sums, axis=0, keepdims=True)

        unroll = 64

        def fetch(step, carry):
            at = step * unroll
            base = map_ref[here * (take // block) + at // block] * block - (at // block) * block
            for k in range(unroll):
                source = pl.multiple_of(row_ref[base + at + k] * parts, parts)
                target = pl.multiple_of((at + k) * parts, parts)
                got_ref[pl.ds(target, parts), :] = wide_ref[pl.ds(source, parts), :]
            return carry

        lax.fori_loop(0, take // unroll, fetch, 0)
        for part in range(parts):
            out_ref[:, part * LANES : (part + 1) * LANES] = got_ref[pl.ds(part, take, stride=parts), :].astype(jnp.bfloat16)

    return pl.pallas_call(
        kernel,
        out_shape=(
            jax.ShapeDtypeStruct((rows, genes), jnp.bfloat16),
            jax.ShapeDtypeStruct((1, genes), jnp.float32),
        ),
        grid_spec=pltpu.PrefetchScalarGridSpec(
            num_scalar_prefetch=2,
            grid=(rows // take,),
            in_specs=[pl.BlockSpec((rows, genes), lambda i, m, r: (0, 0), pipeline_mode=pl.Buffered(1))],
            out_specs=[
                pl.BlockSpec((take, genes), lambda i, m, r: (i, 0)),
                pl.BlockSpec((1, genes), lambda i, m, r: (0, 0)),
            ],
            scratch_shapes=[
                pltpu.VMEM((rows * parts, LANES), jnp.float32),
                pltpu.VMEM((take * parts, LANES), jnp.float32),
            ],
        ),
        cost_estimate=pl.CostEstimate(flops=12 * 10**9, bytes_accessed=4 * rows * genes, transcendentals=0),
        compiler_params=pltpu.CompilerParams(vmem_limit_bytes=34 * 2**20),
        name="match",
    )(block_map, expr_row, expression)


def square_lanes(value):
    wide = value.astype(jnp.float32)
    wide = wide * wide
    total = wide[:, :LANES]
    for part in range(1, wide.shape[1] // LANES):
        total = total + wide[:, part * LANES : (part + 1) * LANES]
    return total


def dot(x, y):
    return jnp.dot(x, y, preferred_element_type=jnp.float32)


def cov_spec(cov):
    array, start, rows = cov
    samples = array.shape[1]
    return pl.BlockSpec((pl.Element(rows), pl.Element(samples)), lambda i: (start, 0))


def over(x, y):
    return lax.dot_general(x, y, (((1,), (1,)), ((), ())), preferred_element_type=jnp.float32)


def fold_in(pieces, covars, matched, slots, width, state, grams):
    count = len(pieces)
    samples = pieces[0].shape[1]
    genes = matched.shape[1]
    covs = covars[0][2]
    tile = 512
    first = state is None
    with_grams = grams is not False
    rows = count * samples // len(slots)
    olds = (() if first else tuple(state)) + (tuple(grams) if with_grams and grams is not None else ())

    def kernel(*refs):
        piece_refs = refs[:count]
        covar_refs = refs[count : 2 * count]
        matched_refs = refs[2 * count : 2 * count + len(slots)]
        rest = refs[2 * count + len(slots) :]
        old_refs = rest[: len(olds)]
        outs = rest[len(olds) :]
        whole = jnp.concatenate([ref[...] for ref in piece_refs], axis=1)
        cov = jnp.concatenate([ref[...] for ref in covar_refs], axis=1)
        mine = jnp.concatenate([ref[...] for ref in matched_refs], axis=0)
        sums = dot(whole, mine)
        loads = over(whole, cov)
        norms = square_lanes(whole)
        if not first:
            sums = sums + old_refs[0][...]
            loads = loads + old_refs[1][...]
            norms = norms + old_refs[2][...]
        outs[0][...] = sums
        outs[1][...] = loads
        outs[2][...] = norms
        if with_grams:

            @pl.when(pl.program_id(0) == 0)
            def _():
                gram = over(cov, cov)
                cross = dot(cov, mine)
                if grams is not None:
                    gram = gram + old_refs[-2][...]
                    cross = cross + old_refs[-1][...]
                outs[3][...] = gram
                outs[4][...] = cross

    piece_spec = pl.BlockSpec((tile, samples), lambda i: (i, 0))
    matched_specs = [pl.BlockSpec((rows, genes), lambda i, slot=slot: (slot, 0)) for slot in slots]
    state_specs = [
        pl.BlockSpec((tile, genes), lambda i: (i, 0)),
        pl.BlockSpec((tile, covs), lambda i: (i, 0)),
        pl.BlockSpec((tile, LANES), lambda i: (i, 0)),
    ]
    gram_specs = [pl.BlockSpec((covs, covs), lambda i: (0, 0)), pl.BlockSpec((covs, genes), lambda i: (0, 0))]
    shapes = [
        jax.ShapeDtypeStruct((width, genes), jnp.float32),
        jax.ShapeDtypeStruct((width, covs), jnp.float32),
        jax.ShapeDtypeStruct((width, LANES), jnp.float32),
    ]
    if with_grams:
        shapes += [jax.ShapeDtypeStruct((covs, covs), jnp.float32), jax.ShapeDtypeStruct((covs, genes), jnp.float32)]
    operands = [*pieces, *[cov[0] for cov in covars], *([matched] * len(slots)), *olds]
    results = pl.pallas_call(
        kernel,
        out_shape=tuple(shapes),
        grid=(width // tile,),
        in_specs=[piece_spec] * count
        + [cov_spec(cov) for cov in covars]
        + matched_specs
        + ([] if first else state_specs)
        + (gram_specs if with_grams and grams is not None else []),
        out_specs=tuple(state_specs + (gram_specs if with_grams else [])),
        input_output_aliases={} if first else {2 * count + len(slots) + k: k for k in range(3)},
        cost_estimate=pl.CostEstimate(
            flops=2 * width * samples * count * (genes + covs), bytes_accessed=8 * width * genes, transcendentals=0
        ),
        compiler_params=pltpu.CompilerParams(vmem_limit_bytes=24 * 2**20),
        name="fold",
    )(*operands)
    return results[:3], results[3:]


def whiten(covars, matched, slots, grams):
    count = len(covars)
    samples = covars[0][0].shape[1]
    genes = matched.shape[1]
    covs = covars[0][2]
    rows = count * samples // len(slots)

    def kernel(*refs):
        covar_refs = refs[:count]
        matched_refs = refs[count : count + len(slots)]
        gram_ref, cross_ref, inverse_ref, loading_ref = refs[count + len(slots) :]
        cov = jnp.concatenate([ref[...] for ref in covar_refs], axis=1)
        mine = jnp.concatenate([ref[...] for ref in matched_refs], axis=0)
        cross = cross_ref[...] + dot(cov, mine)
        left = gram_ref[...] + over(cov, cov)
        row_at = lax.broadcasted_iota(jnp.int32, (covs, covs), 0)
        lane_at = lax.broadcasted_iota(jnp.int32, (covs, covs), 1)
        right = jnp.where(row_at == lane_at, 1.0, 0.0)
        pivots = jnp.zeros((covs, 1), jnp.float32)
        group = 8
        for base in range(0, covs, group):
            live = left[base:, :]
            grown = right[base:, :]
            at = lax.broadcasted_iota(jnp.int32, (covs - base, 1), 0)
            for j in range(group):
                column = live[:, base + j : base + j + 1]
                pivot = live[j : j + 1, base + j : base + j + 1]
                factor = jnp.where(at > j, column / pivot, 0.0)
                live = live - factor * live[j : j + 1, :]
                grown = grown - factor * grown[j : j + 1, :]
            diagonal = jnp.sum(
                jnp.where(
                    lax.broadcasted_iota(jnp.int32, (group, covs), 0) + base
                    == lax.broadcasted_iota(jnp.int32, (group, covs), 1),
                    live[:group, :],
                    0.0,
                ),
                axis=1,
                keepdims=True,
            )
            done = grown[:group, :] * lax.rsqrt(diagonal)
            inverse_ref[base : base + group, :] = done
            if base + group < covs:
                left = jnp.concatenate([left[:base, :], live], axis=0) if base else live
                right = jnp.concatenate([right[:base, :], grown], axis=0) if base else grown
        loading_ref[...] = jnp.dot(inverse_ref[...], cross, precision=lax.Precision.HIGHEST)

    return pl.pallas_call(
        kernel,
        out_shape=(jax.ShapeDtypeStruct((covs, covs), jnp.float32), jax.ShapeDtypeStruct((covs, genes), jnp.float32)),
        grid=(1,),
        in_specs=[cov_spec(cov) for cov in covars]
        + [pl.BlockSpec((rows, genes), lambda i, slot=slot: (slot, 0)) for slot in slots]
        + [pl.BlockSpec((covs, covs), lambda i: (0, 0)), pl.BlockSpec((covs, genes), lambda i: (0, 0))],
        out_specs=(pl.BlockSpec((covs, covs), lambda i: (0, 0)), pl.BlockSpec((covs, genes), lambda i: (0, 0))),
        cost_estimate=pl.CostEstimate(flops=8 * 10**9, bytes_accessed=2 * rows * genes, transcendentals=0),
        compiler_params=pltpu.CompilerParams(vmem_limit_bytes=16 * 2**20),
        name="whiten",
    )(*[cov[0] for cov in covars], *([matched] * len(slots)), *grams)


def finish(full, low, high, covars, matched, slots, state, inverse, loading, panel_norm, scale, out, half, halves):
    count = len(low)
    more = len(full)
    samples = low[0].shape[1]
    genes = matched.shape[1]
    covs = covars[0][2]
    width = state[0].shape[0]
    tile = 512
    steps = width // tile
    split = low[0].shape[0] // tile
    rows = (count + more) * samples // len(slots)
    highest = lax.Precision.HIGHEST

    def kernel(*refs):
        refs = list(refs)

        def take(number):
            taken = refs[:number]
            del refs[:number]
            return taken

        full_refs, low_refs, high_refs, covar_refs = take(more), take(count), take(count), take(more + count)
        matched_refs = take(len(slots))
        sum_ref, load_ref, square_ref, inverse_ref, loading_ref, panel_ref = take(6)
        out_ref = refs[-1]
        here = pl.program_id(0)
        lasts = [jnp.where(here < split, one[...], other[...]) for one, other in zip(low_refs, high_refs)]
        whole = jnp.concatenate([ref[...] for ref in full_refs] + lasts, axis=1)
        cov = jnp.concatenate([ref[...] for ref in covar_refs], axis=1)
        mine = jnp.concatenate([ref[...] for ref in matched_refs], axis=0)
        sums = sum_ref[...] + dot(whole, mine)
        loads = load_ref[...] + over(whole, cov)
        squares = jnp.sum(square_ref[...] + square_lanes(whole), axis=1, keepdims=True)
        white = lax.dot_general(loads, inverse_ref[...], (((1,), (1,)), ((), ())), precision=highest)
        fitted = jnp.dot(white, loading_ref[...], precision=highest)
        resid_norm = jnp.maximum(squares - jnp.sum(white * white, axis=1, keepdims=True), 0.0)
        gain = scale * lax.rsqrt(resid_norm + epsilon)
        out_ref[...] = (sums - fitted) * gain * lax.rsqrt(panel_ref[...] + epsilon)

    operands = [*full, *low, *high, *[cov[0] for cov in covars], *([matched] * len(slots))]
    operands += [*state, inverse, loading, panel_norm]
    in_specs = (
        [pl.BlockSpec((tile, samples), lambda i: (i, 0))] * more
        + [pl.BlockSpec((tile, samples), lambda i: (jnp.minimum(i, split - 1), 0))] * count
        + [pl.BlockSpec((tile, samples), lambda i: (jnp.maximum(i - split, 0), 0))] * count
        + [cov_spec(cov) for cov in covars]
        + [pl.BlockSpec((rows, genes), lambda i, slot=slot: (slot, 0)) for slot in slots]
        + [
            pl.BlockSpec((tile, genes), lambda i: (i, 0)),
            pl.BlockSpec((tile, covs), lambda i: (i, 0)),
            pl.BlockSpec((tile, LANES), lambda i: (i, 0)),
            pl.BlockSpec((covs, covs), lambda i: (0, 0)),
            pl.BlockSpec((covs, genes), lambda i: (0, 0)),
            pl.BlockSpec((1, genes), lambda i: (0, 0)),
        ]
    )
    aliases = {}
    if out is not None:
        aliases = {len(operands): 0}
        operands.append(out)
        in_specs.append(pl.BlockSpec(memory_space=pl.ANY))
    return pl.pallas_call(
        kernel,
        out_shape=jax.ShapeDtypeStruct((halves * width, genes), jnp.float32),
        grid=(steps,),
        in_specs=in_specs,
        out_specs=pl.BlockSpec((tile, genes), lambda i: (half * steps + i, 0)),
        input_output_aliases=aliases,
        cost_estimate=pl.CostEstimate(
            flops=2 * width * samples * (count + more) * genes + 14 * width * covs * genes,
            bytes_accessed=8 * width * genes,
            transcendentals=0,
        ),
        compiler_params=pltpu.CompilerParams(vmem_limit_bytes=20 * 2**20),
        name="finish",
    )(*operands)


def whole(dosage, covariates, expression, block_index, expr_row):
    blocks = block_index.shape[0]
    covars = covariates.shape[1]
    here = dosage.shape[0]
    ring = lax.axis_size("samp_0")
    turns = ring // 2
    chip = lax.axis_index("samp_0")
    core = lax.axis_index("samp_1")
    scale = math.sqrt(expr_row.shape[0] - covars - 1)
    up = [(i, (i + 1) % ring) for i in range(ring)]
    down = [(i, (i - 1) % ring) for i in range(ring)]
    cross = [(0, 1), (1, 0)]

    def swap(x):
        return lax.ppermute(x, "samp_1", cross)

    order = [chip]
    for turn in range(1, turns):
        order += [chip - turn, chip + turn]
    order += [chip + turns]
    order = [chip_at % ring for chip_at in order]
    block_map = jnp.stack([2 * chip_at + side for chip_at in order for side in (core, 1 - core)]).astype(jnp.int32)

    def pair_of(up_value, down_value):
        return (up_value, swap(up_value), down_value, swap(down_value))

    def shift(values, turn):
        up_value, down_value = values
        if turn == turns:
            middle = width // 2
            up_value, down_value = up_value[:middle], down_value[middle:width]
        up_value = lax.ppermute(up_value, "samp_0", up)
        down_value = lax.ppermute(down_value, "samp_0", down)
        return up_value, down_value

    width = block_index.shape[1]
    own_cov = covariates.T
    next_cov = shift((own_cov, own_cov), 0)
    flow = [None] * blocks
    arrived = [{} for _ in range(blocks)]
    for block in range(blocks):
        pieces = pick_columns(dosage, block_index, block, next_cov if block == 0 else ())
        flow[block] = (pieces[0], pieces[-1])
        arrived[block][0] = (pieces[0], swap(pieces[0]))
    first_covs = jnp.concatenate([own_cov, *next_cov], axis=0)
    first_swap = swap(first_covs)
    covs = {
        0: tuple((array, 0, covars) for array in (first_covs, first_swap)),
        1: tuple((array, k * covars, covars) for k in (1, 2) for array in (first_covs, first_swap)),
    }
    matched, panel_norm = match_rows(expression, expr_row, block_map, here)

    def inputs(turns_here, block):
        slots = []
        pieces = []
        covars_here = []
        for turn in turns_here:
            slots += [0] if turn == 0 else [2 * turn - 1, 2 * turn]
            pieces += arrived[block][turn]
            covars_here += covs[turn]
        return tuple(pieces), tuple(covars_here), matched, tuple(slots), width

    state = [None] * blocks
    grams = None
    for turn in range(1, turns):
        for block in range(blocks):
            flow[block] = shift(flow[block], turn)
            arrived[block][turn] = pair_of(*flow[block])
            if block == 0:
                riders = tuple((array, width, covars) for array in arrived[0][turn])
                covs[turn + 1] = riders if turn + 1 < turns else riders[:2]
            if turn % 2 == 0:
                ready = (0, 1, 2) if turn == 2 else (turn - 1, turn)
                state[block], summed = fold_in(
                    *inputs(ready, block), state[block], grams if block == 0 else False
                )
                if block == 0:
                    grams = summed

    rest = (*covs[turns - 1], *covs[turns])
    last_slots = tuple(range(2 * turns - 3, 2 * turns))
    inverse, loading = whiten(rest, matched, last_slots, grams)

    out = None
    for block in range(blocks):
        flow[block] = shift(flow[block], turns)
        low, low_swap, high, high_swap = pair_of(*flow[block])
        out = finish(
            arrived[block][turns - 1],
            (low, low_swap),
            (high, high_swap),
            rest,
            matched,
            last_slots,
            state[block],
            inverse,
            loading,
            panel_norm,
            scale,
            out,
            block,
            blocks,
        )
    return out


def solution(mesh):
    torus = Mesh(mesh.devices.reshape(mesh.shape["groups"], -1, 2), ("groups", "samp_0", "samp_1"))
    in_specs = (
        P(GROUPS_SAMP, None),
        P(GROUPS_SAMP, None),
        P("groups", SAMP),
        P("groups", None),
        P("groups"),
    )
    out_specs = P("groups", SAMP)
    return jax.shard_map(whole, mesh=torus, in_specs=in_specs, out_specs=out_specs, check_vma=False)
```

```python
import math

import jax
import jax.numpy as jnp
from jax import lax
from jax.experimental import pallas as pl
from jax.experimental.pallas import tpu as pltpu
from jax.sharding import Mesh
from jax.sharding import PartitionSpec as P


GROUPS_SAMP = ("groups", "samp_0", "samp_1")
SAMP = ("samp_0", "samp_1")
LANES = 128

epsilon = 1e-06


def pick_columns(dosage, block_index, block, extra, copies):
    samples, panel = dosage.shape
    blocks, width = block_index.shape
    span = 2048
    tile = 512
    spans = panel // span
    tiles = width // tile

    def kernel(index_ref, dosage_ref, *refs):
        index_at_ref, even_ref, odd_ref, sum_ref = refs[copies:]
        lane = lax.broadcasted_iota(jnp.int32, (LANES, LANES), 1)
        for part in range(width // LANES):
            row = index_ref[block : block + 1, part * LANES : (part + 1) * LANES].astype(jnp.float32)
            index_at_ref[part * LANES : (part + 1) * LANES, :] = (
                jnp.broadcast_to(row, (LANES, LANES)).T.astype(jnp.int32) - lane
            )

        def build(item, hot_ref):
            rows = pl.ds(pl.multiple_of((item // spans) * tile, tile), tile)
            column = index_at_ref[rows, :] - (item % spans) * span
            for step in range(span // LANES):
                hot_ref[:, step * LANES : (step + 1) * LANES] = jnp.where(column == step * LANES, 1.0, 0.0).astype(
                    jnp.bfloat16
                )

        def add(item, hot_ref):
            rows = pl.ds(pl.multiple_of((item // spans) * tile, tile), tile)
            span_at = item % spans
            columns = pl.ds(pl.multiple_of(span_at * span, span), span)
            picked = over(hot_ref[...], dosage_ref[:, columns])
            sum_ref[rows, :] = jnp.where(span_at == 0, 0.0, sum_ref[rows, :]) + picked

        def step(pair, carry):
            item = 2 * pair

            add(item, even_ref)
            build(item + 1, odd_ref)
            add(item + 1, odd_ref)
            build(jnp.minimum(item + 2, tiles * spans - 1), even_ref)
            return carry

        build(0, even_ref)
        lax.fori_loop(0, tiles * spans // 2, step, 0)
        for out_ref in refs[:copies]:
            out_ref[:width, :] = sum_ref[...].astype(jnp.bfloat16)

    return pl.pallas_call(
        kernel,
        out_shape=(jax.ShapeDtypeStruct((width + extra, samples), jnp.bfloat16),) * copies,
        grid=(1,),
        in_specs=[pl.BlockSpec((blocks, width), lambda i: (0, 0)), pl.BlockSpec((samples, panel), lambda i: (0, 0))],
        out_specs=(pl.BlockSpec((width + extra, samples), lambda i: (0, 0)),) * copies,
        scratch_shapes=[
            pltpu.VMEM((width, LANES), jnp.int32),
            pltpu.VMEM((tile, span), jnp.bfloat16),
            pltpu.VMEM((tile, span), jnp.bfloat16),
            pltpu.VMEM((width, samples), jnp.float32),
        ],
        cost_estimate=pl.CostEstimate(flops=2 * width * samples * panel, bytes_accessed=2 * samples * panel, transcendentals=0),
        compiler_params=pltpu.CompilerParams(vmem_limit_bytes=20 * 2**20),
        name="pick",
    )(block_index, dosage)


def ride(arrays, riders, width):
    count = len(arrays)
    rows, samples = riders[0].shape

    def kernel(*refs):
        for rider_ref, out_ref in zip(refs[count : 2 * count], refs[2 * count :]):
            out_ref[...] = rider_ref[...]

    block = pl.BlockSpec((pl.Element(rows), pl.Element(samples)), lambda i: (width, 0))
    return pl.pallas_call(
        kernel,
        out_shape=tuple(jax.ShapeDtypeStruct(array.shape, array.dtype) for array in arrays),
        grid=(1,),
        in_specs=[pl.BlockSpec(memory_space=pl.ANY)] * count + [pl.BlockSpec((rows, samples), lambda i: (0, 0))] * count,
        out_specs=(block,) * count,
        input_output_aliases={k: k for k in range(count)},
        compiler_params=pltpu.CompilerParams(vmem_limit_bytes=8 * 2**20),
        name="ride",
    )(*arrays, *riders)


def match_rows(expression, expr_row, block_map, block, first, count, with_norm):
    rows, genes = expression.shape
    parts = genes // LANES
    chunk = 128
    take = 4 * block

    share = count * block

    def kernel(map_ref, row_ref, exp_ref, out_ref, *refs):
        wide_ref, got_ref = refs[-2:]
        here = pl.program_id(0)

        @pl.when(here == 0)
        def _():
            def widen(step, sums):
                at = pl.multiple_of(step * chunk, chunk)
                value = exp_ref[pl.ds(at, chunk), :].astype(jnp.float32)
                for part in range(parts):
                    wide_ref[pl.ds(at * parts + part, chunk, stride=parts), :] = value[:, part * LANES : (part + 1) * LANES]
                if not with_norm:
                    return sums
                square = value * value
                return sums + jnp.sum(square.reshape(chunk // 8, 8, genes), axis=0)

            sums = lax.fori_loop(0, rows // chunk, widen, jnp.zeros((8, genes), jnp.float32))
            if with_norm:
                refs[0][...] = jnp.sum(sums, axis=0, keepdims=True)

        unroll = 64

        def fetch(step, carry):
            at = step * unroll
            base = map_ref[first + here * (take // block) + at // block] * block - (at // block) * block
            for k in range(unroll):
                source = pl.multiple_of(row_ref[base + at + k] * parts, parts)
                target = pl.multiple_of((at + k) * parts, parts)
                got_ref[pl.ds(target, parts), :] = wide_ref[pl.ds(source, parts), :]
            return carry

        lax.fori_loop(0, take // unroll, fetch, 0)

        def narrow(step, carry):
            at = pl.multiple_of(step * chunk, chunk)
            for part in range(parts):
                value = got_ref[pl.ds(at * parts + part, chunk, stride=parts), :]
                out_ref[pl.ds(at, chunk), part * LANES : (part + 1) * LANES] = value.astype(jnp.bfloat16)
            return carry

        lax.fori_loop(0, take // chunk, narrow, 0)

    norm_shape = (jax.ShapeDtypeStruct((1, genes), jnp.float32),) if with_norm else ()
    norm_spec = [pl.BlockSpec((1, genes), lambda i, m, r: (0, 0))] if with_norm else []
    return pl.pallas_call(
        kernel,
        out_shape=(jax.ShapeDtypeStruct((share, genes), jnp.bfloat16), *norm_shape),
        grid_spec=pltpu.PrefetchScalarGridSpec(
            num_scalar_prefetch=2,
            grid=(share // take,),
            in_specs=[pl.BlockSpec((rows, genes), lambda i, m, r: (0, 0), pipeline_mode=pl.Buffered(1))],
            out_specs=[pl.BlockSpec((take, genes), lambda i, m, r: (i, 0)), *norm_spec],
            scratch_shapes=[
                pltpu.VMEM((rows * parts, LANES), jnp.float32),
                pltpu.VMEM((take * parts, LANES), jnp.float32),
            ],
        ),
        cost_estimate=pl.CostEstimate(flops=8 * 10**9, bytes_accessed=4 * rows * genes, transcendentals=0),
        compiler_params=pltpu.CompilerParams(vmem_limit_bytes=34 * 2**20),
        name="match",
    )(block_map, expr_row, expression)


def split_terms(value):
    high = value.astype(jnp.bfloat16)
    rest = value - high.astype(jnp.float32)
    middle = rest.astype(jnp.bfloat16)
    low = (rest - middle.astype(jnp.float32)).astype(jnp.bfloat16)
    return high, middle, low


def spread_left(value, axis):
    high, middle, low = split_terms(value)
    return jnp.concatenate([high, high, middle, high, middle, low], axis=axis)


def spread_right(value, axis):
    high, middle, low = split_terms(value)
    return jnp.concatenate([high, middle, high, low, middle, high], axis=axis)


def slot_specs(matched, slots, rows, genes):
    half = matched[0].shape[0] // rows
    arrays = [matched[slot // half] for slot in slots]
    return arrays, [pl.BlockSpec((rows, genes), lambda i, slot=slot: (slot % half, 0)) for slot in slots]


def square_lanes(value):
    wide = value.astype(jnp.float32)
    wide = wide * wide
    total = wide[:, :LANES]
    for part in range(1, wide.shape[1] // LANES):
        total = total + wide[:, part * LANES : (part + 1) * LANES]
    return total


def dot(x, y):
    return jnp.dot(x, y, preferred_element_type=jnp.float32)


def cov_spec(cov):
    array, start, rows = cov
    samples = array.shape[1]
    return pl.BlockSpec((pl.Element(rows), pl.Element(samples)), lambda i: (start, 0))


def over(x, y):
    return lax.dot_general(x, y, (((1,), (1,)), ((), ())), preferred_element_type=jnp.float32)


def fold_in(pieces, covars, matched, slots, width, state, grams):
    count = len(pieces)
    samples = pieces[0].shape[1]
    genes = matched[0].shape[1]
    covs = covars[0][2]
    tile = 256
    first = state is None
    with_grams = grams is not False
    rows = count * samples // len(slots)
    olds = (() if first else tuple(state)) + (tuple(grams) if with_grams and grams is not None else ())

    def kernel(*refs):
        piece_refs = refs[:count]
        covar_refs = refs[count : 2 * count]
        matched_refs = refs[2 * count : 2 * count + len(slots)]
        rest = refs[2 * count + len(slots) :]
        old_refs = rest[: len(olds)]
        outs = rest[len(olds) :]
        whole = jnp.concatenate([ref[...] for ref in piece_refs], axis=1)
        cov = jnp.concatenate([ref[...] for ref in covar_refs], axis=1)
        mine = jnp.concatenate([ref[...] for ref in matched_refs], axis=0)
        sums = dot(whole, mine)
        loads = over(whole, cov)
        norms = square_lanes(whole)
        if not first:
            sums = sums + old_refs[0][...]
            loads = loads + old_refs[1][...]
            norms = norms + old_refs[2][...]
        outs[0][...] = sums
        outs[1][...] = loads
        outs[2][...] = norms
        if with_grams:

            @pl.when(pl.program_id(0) == 0)
            def _():
                gram = over(cov, cov)
                cross = dot(cov, mine)
                if grams is not None:
                    gram = gram + old_refs[-2][...]
                    cross = cross + old_refs[-1][...]
                outs[3][...] = gram
                outs[4][...] = cross

    piece_spec = pl.BlockSpec((tile, samples), lambda i: (i, 0))
    matched_arrays, matched_specs = slot_specs(matched, slots, rows, genes)
    state_specs = [
        pl.BlockSpec((tile, genes), lambda i: (i, 0)),
        pl.BlockSpec((tile, covs), lambda i: (i, 0)),
        pl.BlockSpec((tile, LANES), lambda i: (i, 0)),
    ]
    gram_specs = [pl.BlockSpec((covs, covs), lambda i: (0, 0)), pl.BlockSpec((covs, genes), lambda i: (0, 0))]
    shapes = [
        jax.ShapeDtypeStruct((width, genes), jnp.float32),
        jax.ShapeDtypeStruct((width, covs), jnp.float32),
        jax.ShapeDtypeStruct((width, LANES), jnp.float32),
    ]
    if with_grams:
        shapes += [jax.ShapeDtypeStruct((covs, covs), jnp.float32), jax.ShapeDtypeStruct((covs, genes), jnp.float32)]
    operands = [*pieces, *[cov[0] for cov in covars], *matched_arrays, *olds]
    results = pl.pallas_call(
        kernel,
        out_shape=tuple(shapes),
        grid=(width // tile,),
        in_specs=[piece_spec] * count
        + [cov_spec(cov) for cov in covars]
        + matched_specs
        + ([] if first else state_specs)
        + (gram_specs if with_grams and grams is not None else []),
        out_specs=tuple(state_specs + (gram_specs if with_grams else [])),
        input_output_aliases={} if first else {2 * count + len(slots) + k: k for k in range(3)},
        cost_estimate=pl.CostEstimate(
            flops=2 * width * samples * count * (genes + covs), bytes_accessed=8 * width * genes, transcendentals=0
        ),
        compiler_params=pltpu.CompilerParams(vmem_limit_bytes=24 * 2**20),
        name="fold",
    )(*operands)
    return results[:3], results[3:]


def whiten(covars, matched, slots, grams):
    count = len(covars)
    samples = covars[0][0].shape[1]
    genes = matched[0].shape[1]
    covs = covars[0][2]
    rows = count * samples // len(slots)
    matched_arrays, matched_specs = slot_specs(matched, slots, rows, genes)

    def kernel(*refs):
        covar_refs = refs[:count]
        matched_refs = refs[count : count + len(slots)]
        gram_ref, cross_ref, inverse_ref, loading_ref = refs[count + len(slots) :]
        cov = jnp.concatenate([ref[...] for ref in covar_refs], axis=1)
        mine = jnp.concatenate([ref[...] for ref in matched_refs], axis=0)
        cross = cross_ref[...] + dot(cov, mine)
        gram = gram_ref[...] + over(cov, cov)
        pad = jnp.zeros((covs, LANES - covs), jnp.float32)
        row_at = lax.broadcasted_iota(jnp.int32, (covs, LANES), 0)
        lane_at = lax.broadcasted_iota(jnp.int32, (covs, LANES), 1)
        at = lax.broadcasted_iota(jnp.int32, (covs, 1), 0)
        group = 8

        def eliminate(turn, pair):
            live, grown = pair
            undone = at < covs - turn * group
            for j in range(group):
                factor = jnp.where((at > j) & undone, live[:, j : j + 1] * (1.0 / live[j : j + 1, j : j + 1]), 0.0)
                live = live - factor * live[j : j + 1, :]
                grown = grown - factor * grown[j : j + 1, :]
            diagonal = jnp.sum(
                jnp.where(row_at[:group, :] == lane_at[:group, :], live[:group, :], 0.0), axis=1, keepdims=True
            )
            done = grown[:group, :] * lax.rsqrt(diagonal)
            inverse_ref[pl.ds(pl.multiple_of(turn * group, group), group), :] = done[:, :covs]
            live = pltpu.roll(jnp.concatenate([live[group:, :], live[:group, :]], axis=0), LANES - group, 1)
            grown = jnp.concatenate([grown[group:, :], grown[:group, :]], axis=0)
            return live, grown

        pair = (jnp.concatenate([gram, pad], axis=1), jnp.where(row_at == lane_at, 1.0, 0.0))
        lax.fori_loop(0, covs // group, eliminate, pair)
        loading_ref[...] = jnp.dot(inverse_ref[...], cross, precision=lax.Precision.HIGHEST)

    return pl.pallas_call(
        kernel,
        out_shape=(jax.ShapeDtypeStruct((covs, covs), jnp.float32), jax.ShapeDtypeStruct((covs, genes), jnp.float32)),
        grid=(1,),
        in_specs=[cov_spec(cov) for cov in covars]
        + matched_specs
        + [pl.BlockSpec((covs, covs), lambda i: (0, 0)), pl.BlockSpec((covs, genes), lambda i: (0, 0))],
        out_specs=(pl.BlockSpec((covs, covs), lambda i: (0, 0)), pl.BlockSpec((covs, genes), lambda i: (0, 0))),
        cost_estimate=pl.CostEstimate(flops=8 * 10**9, bytes_accessed=2 * rows * genes, transcendentals=0),
        compiler_params=pltpu.CompilerParams(vmem_limit_bytes=16 * 2**20),
        name="whiten",
    )(*[cov[0] for cov in covars], *matched_arrays, *grams)


def finish(full, low, high, covars, matched, slots, state, inverse, loading, panel_norm, scale, out, half, halves):
    count = len(low)
    more = len(full)
    samples = low[0].shape[1]
    genes = matched[0].shape[1]
    covs = covars[0][2]
    width = state[0].shape[0]
    tile = 512
    steps = width // tile
    split = low[0].shape[0] // tile
    rows = (count + more) * samples // len(slots)
    matched_arrays, matched_specs = slot_specs(matched, slots, rows, genes)

    def kernel(*refs):
        refs = list(refs)

        def take(number):
            taken = refs[:number]
            del refs[:number]
            return taken

        full_refs, low_refs, high_refs, covar_refs = take(more), take(count), take(count), take(more + count)
        matched_refs = take(len(slots))
        sum_ref, load_ref, square_ref, inverse_ref, loading_ref, panel_ref = take(6)
        out_ref = refs[-1]
        here = pl.program_id(0)
        lasts = [jnp.where(here < split, one[...], other[...]) for one, other in zip(low_refs, high_refs)]
        whole = jnp.concatenate([ref[...] for ref in full_refs] + lasts, axis=1)
        cov = jnp.concatenate([ref[...] for ref in covar_refs], axis=1)
        mine = jnp.concatenate([ref[...] for ref in matched_refs], axis=0)
        sums = sum_ref[...] + dot(whole, mine)
        loads = load_ref[...] + over(whole, cov)
        squares = jnp.sum(square_ref[...] + square_lanes(whole), axis=1, keepdims=True)
        white = over(spread_left(loads, 1), spread_right(inverse_ref[...], 1))
        fitted = dot(spread_left(white, 1), spread_right(loading_ref[...], 0))
        resid_norm = jnp.maximum(squares - jnp.sum(white * white, axis=1, keepdims=True), 0.0)
        gain = scale * lax.rsqrt(resid_norm + epsilon)
        out_ref[...] = (sums - fitted) * gain * lax.rsqrt(panel_ref[...] + epsilon)

    operands = [*full, *low, *high, *[cov[0] for cov in covars], *matched_arrays]
    operands += [*state, inverse, loading, panel_norm]
    in_specs = (
        [pl.BlockSpec((tile, samples), lambda i: (i, 0))] * more
        + [pl.BlockSpec((tile, samples), lambda i: (jnp.minimum(i, split - 1), 0))] * count
        + [pl.BlockSpec((tile, samples), lambda i: (jnp.maximum(i - split, 0), 0))] * count
        + [cov_spec(cov) for cov in covars]
        + matched_specs
        + [
            pl.BlockSpec((tile, genes), lambda i: (i, 0)),
            pl.BlockSpec((tile, covs), lambda i: (i, 0)),
            pl.BlockSpec((tile, LANES), lambda i: (i, 0)),
            pl.BlockSpec((covs, covs), lambda i: (0, 0)),
            pl.BlockSpec((covs, genes), lambda i: (0, 0)),
            pl.BlockSpec((1, genes), lambda i: (0, 0)),
        ]
    )
    aliases = {}
    if out is not None:
        aliases = {len(operands): 0}
        operands.append(out)
        in_specs.append(pl.BlockSpec(memory_space=pl.ANY))
    return pl.pallas_call(
        kernel,
        out_shape=jax.ShapeDtypeStruct((halves * width, genes), jnp.float32),
        grid=(steps,),
        in_specs=in_specs,
        out_specs=pl.BlockSpec((tile, genes), lambda i: (half * steps + i, 0)),
        input_output_aliases=aliases,
        cost_estimate=pl.CostEstimate(
            flops=2 * width * samples * (count + more) * genes + 14 * width * covs * genes,
            bytes_accessed=8 * width * genes,
            transcendentals=0,
        ),
        compiler_params=pltpu.CompilerParams(vmem_limit_bytes=20 * 2**20),
        name="finish",
    )(*operands)


def whole(dosage, covariates, expression, block_index, expr_row):
    blocks = block_index.shape[0]
    covars = covariates.shape[1]
    here = dosage.shape[0]
    ring = lax.axis_size("samp_0")
    turns = ring // 2
    chip = lax.axis_index("samp_0")
    core = lax.axis_index("samp_1")
    scale = math.sqrt(expr_row.shape[0] - covars - 1)
    up = [(i, (i + 1) % ring) for i in range(ring)]
    down = [(i, (i - 1) % ring) for i in range(ring)]
    cross = [(0, 1), (1, 0)]

    def swap(x):
        return lax.ppermute(x, "samp_1", cross)

    order = [chip]
    for turn in range(1, turns):
        order += [chip - turn, chip + turn]
    order += [chip + turns]
    order = [chip_at % ring for chip_at in order]
    block_map = jnp.stack([2 * chip_at + side for chip_at in order for side in (core, 1 - core)]).astype(jnp.int32)

    def pair_of(up_value, down_value):
        return (up_value, swap(up_value), down_value, swap(down_value))

    def shift(values, turn):
        up_value, down_value = values
        if turn == turns:
            middle = width // 2
            up_value, down_value = up_value[:middle], down_value[middle:width]
        up_value = lax.ppermute(up_value, "samp_0", up)
        down_value = lax.ppermute(down_value, "samp_0", down)
        return up_value, down_value

    width = block_index.shape[1]
    own_cov = covariates.T
    next_cov = shift((own_cov, own_cov), 0)
    flow = [None] * blocks
    arrived = [{} for _ in range(blocks)]
    for block in range(blocks):
        if block == 0:
            pieces = pick_columns(dosage, block_index, block, covars, 2)
        else:
            pieces = pick_columns(dosage, block_index, block, 0, 1)
        if block == 0:
            pieces = ride(pieces, next_cov, width)
        flow[block] = (pieces[0], pieces[-1])
        arrived[block][0] = (pieces[0], swap(pieces[0]))
    first_covs = jnp.concatenate([own_cov, *next_cov], axis=0)
    first_swap = swap(first_covs)
    covs = {
        0: tuple((array, 0, covars) for array in (first_covs, first_swap)),
        1: tuple((array, k * covars, covars) for k in (1, 2) for array in (first_covs, first_swap)),
    }
    middle = block_map.shape[0] // 2
    first_rows, panel_norm = match_rows(expression, expr_row, block_map, here, 0, middle, True)
    (last_rows,) = match_rows(expression, expr_row, block_map, here, middle, middle, False)
    matched = (first_rows, last_rows)

    def inputs(turns_here, block):
        slots = []
        pieces = []
        covars_here = []
        for turn in turns_here:
            slots += [0] if turn == 0 else [2 * turn - 1, 2 * turn]
            pieces += arrived[block][turn]
            covars_here += covs[turn]
        return tuple(pieces), tuple(covars_here), matched, tuple(slots), width

    state = [None] * blocks
    grams = None
    for turn in range(1, turns):
        for block in range(blocks):
            flow[block] = shift(flow[block], turn)
            arrived[block][turn] = pair_of(*flow[block])
            if block == 0:
                riders = tuple((array, width, covars) for array in arrived[0][turn])
                covs[turn + 1] = riders if turn + 1 < turns else riders[:2]
            if turn % 2 == 0:
                ready = (0, 1, 2) if turn == 2 else (turn - 1, turn)
                state[block], summed = fold_in(
                    *inputs(ready, block), state[block], grams if block == 0 else False
                )
                if block == 0:
                    grams = summed

    rest = (*covs[turns - 1], *covs[turns])
    last_slots = tuple(range(2 * turns - 3, 2 * turns))
    inverse, loading = whiten(rest, matched, last_slots, grams)

    out = None
    for block in range(blocks):
        flow[block] = shift(flow[block], turns)
        low, low_swap, high, high_swap = pair_of(*flow[block])
        out = finish(
            arrived[block][turns - 1],
            (low, low_swap),
            (high, high_swap),
            rest,
            matched,
            last_slots,
            state[block],
            inverse,
            loading,
            panel_norm,
            scale,
            out,
            block,
            blocks,
        )
    return out


def solution(mesh):
    torus = Mesh(mesh.devices.reshape(mesh.shape["groups"], -1, 2), ("groups", "samp_0", "samp_1"))
    in_specs = (
        P(GROUPS_SAMP, None),
        P(GROUPS_SAMP, None),
        P("groups", SAMP),
        P("groups", None),
        P("groups"),
    )
    out_specs = P("groups", SAMP)
    return jax.shard_map(whole, mesh=torus, in_specs=in_specs, out_specs=out_specs, check_vma=False)
```

```python
import math

import jax
import jax.numpy as jnp
from jax import lax
from jax.experimental import pallas as pl
from jax.experimental.pallas import tpu as pltpu
from jax.sharding import Mesh
from jax.sharding import PartitionSpec as P


GROUPS_SAMP = ("groups", "samp_0", "samp_1")
SAMP = ("samp_0", "samp_1")
LANES = 128

epsilon = 1e-06


def pick_columns(dosage, block_index, block, extra, copies):
    samples, panel = dosage.shape
    blocks, width = block_index.shape
    span = 2048
    tile = 512
    spans = panel // span
    tiles = width // tile

    def kernel(index_ref, dosage_ref, *refs):
        index_at_ref, even_ref, odd_ref, sum_ref = refs[copies:]
        lane = lax.broadcasted_iota(jnp.int32, (LANES, LANES), 1)
        for part in range(width // LANES):
            row = index_ref[block : block + 1, part * LANES : (part + 1) * LANES].astype(jnp.float32)
            index_at_ref[part * LANES : (part + 1) * LANES, :] = (
                jnp.broadcast_to(row, (LANES, LANES)).T.astype(jnp.int32) - lane
            )

        def build(item, hot_ref):
            rows = pl.ds(pl.multiple_of((item // spans) * tile, tile), tile)
            column = index_at_ref[rows, :] - (item % spans) * span
            for step in range(span // LANES):
                hot_ref[:, step * LANES : (step + 1) * LANES] = jnp.where(column == step * LANES, 1.0, 0.0).astype(
                    jnp.bfloat16
                )

        def add(item, hot_ref):
            rows = pl.ds(pl.multiple_of((item // spans) * tile, tile), tile)
            span_at = item % spans
            columns = pl.ds(pl.multiple_of(span_at * span, span), span)
            picked = over(hot_ref[...], dosage_ref[:, columns])
            sum_ref[rows, :] = jnp.where(span_at == 0, 0.0, sum_ref[rows, :]) + picked

        def step(pair, carry):
            item = 2 * pair

            add(item, even_ref)
            build(item + 1, odd_ref)
            add(item + 1, odd_ref)
            build(jnp.minimum(item + 2, tiles * spans - 1), even_ref)
            return carry

        build(0, even_ref)
        lax.fori_loop(0, tiles * spans // 2, step, 0)
        for out_ref in refs[:copies]:
            out_ref[:width, :] = sum_ref[...].astype(jnp.bfloat16)

    return pl.pallas_call(
        kernel,
        out_shape=(jax.ShapeDtypeStruct((width + extra, samples), jnp.bfloat16),) * copies,
        grid=(1,),
        in_specs=[pl.BlockSpec((blocks, width), lambda i: (0, 0)), pl.BlockSpec((samples, panel), lambda i: (0, 0))],
        out_specs=(pl.BlockSpec((width + extra, samples), lambda i: (0, 0)),) * copies,
        scratch_shapes=[
            pltpu.VMEM((width, LANES), jnp.int32),
            pltpu.VMEM((tile, span), jnp.bfloat16),
            pltpu.VMEM((tile, span), jnp.bfloat16),
            pltpu.VMEM((width, samples), jnp.float32),
        ],
        cost_estimate=pl.CostEstimate(flops=2 * width * samples * panel, bytes_accessed=2 * samples * panel, transcendentals=0),
        compiler_params=pltpu.CompilerParams(vmem_limit_bytes=20 * 2**20),
        name="pick",
    )(block_index, dosage)


def ride(arrays, riders, width):
    count = len(arrays)
    rows, samples = riders[0].shape

    def kernel(*refs):
        for rider_ref, out_ref in zip(refs[count : 2 * count], refs[2 * count :]):
            out_ref[...] = rider_ref[...]

    block = pl.BlockSpec((pl.Element(rows), pl.Element(samples)), lambda i: (width, 0))
    return pl.pallas_call(
        kernel,
        out_shape=tuple(jax.ShapeDtypeStruct(array.shape, array.dtype) for array in arrays),
        grid=(1,),
        in_specs=[pl.BlockSpec(memory_space=pl.ANY)] * count + [pl.BlockSpec((rows, samples), lambda i: (0, 0))] * count,
        out_specs=(block,) * count,
        input_output_aliases={k: k for k in range(count)},
        compiler_params=pltpu.CompilerParams(vmem_limit_bytes=8 * 2**20),
        name="ride",
    )(*arrays, *riders)


def join(arrays):
    samples = arrays[0].shape[1]
    starts = [0]
    for array in arrays:
        starts.append(starts[-1] + array.shape[0])

    def kernel(*refs):
        for ref, start in zip(refs[:-1], starts):
            refs[-1][start : start + ref.shape[0], :] = ref[...]

    joined = pl.pallas_call(
        kernel,
        out_shape=jax.ShapeDtypeStruct((starts[-1], samples), arrays[0].dtype),
        grid=(1,),
        in_specs=[pl.BlockSpec(array.shape, lambda i: (0, 0)) for array in arrays],
        out_specs=pl.BlockSpec((starts[-1], samples), lambda i: (0, 0)),
        compiler_params=pltpu.CompilerParams(vmem_limit_bytes=20 * 2**20),
        name="join",
    )(*arrays)
    return joined, starts[:-1]


def match_rows(expression, expr_row, block_map, block, first, count, with_norm):
    rows, genes = expression.shape
    parts = genes // LANES
    chunk = 128
    take = 4 * block

    share = count * block

    def kernel(map_ref, row_ref, exp_ref, out_ref, *refs):
        wide_ref, got_ref = refs[-2:]
        here = pl.program_id(0)

        @pl.when(here == 0)
        def _():
            def widen(step, sums):
                at = pl.multiple_of(step * chunk, chunk)
                value = exp_ref[pl.ds(at, chunk), :].astype(jnp.float32)
                for part in range(parts):
                    wide_ref[pl.ds(at * parts + part, chunk, stride=parts), :] = value[:, part * LANES : (part + 1) * LANES]
                if not with_norm:
                    return sums
                square = value * value
                return sums + jnp.sum(square.reshape(chunk // 8, 8, genes), axis=0)

            sums = lax.fori_loop(0, rows // chunk, widen, jnp.zeros((8, genes), jnp.float32))
            if with_norm:
                refs[0][...] = jnp.sum(sums, axis=0, keepdims=True)

        unroll = 64

        def fetch(step, carry):
            at = step * unroll
            base = map_ref[first + here * (take // block) + at // block] * block - (at // block) * block
            for k in range(unroll):
                source = pl.multiple_of(row_ref[base + at + k] * parts, parts)
                target = pl.multiple_of((at + k) * parts, parts)
                got_ref[pl.ds(target, parts), :] = wide_ref[pl.ds(source, parts), :]
            return carry

        lax.fori_loop(0, take // unroll, fetch, 0)

        def narrow(step, carry):
            at = pl.multiple_of(step * chunk, chunk)
            for part in range(parts):
                value = got_ref[pl.ds(at * parts + part, chunk, stride=parts), :]
                out_ref[pl.ds(at, chunk), part * LANES : (part + 1) * LANES] = value.astype(jnp.bfloat16)
            return carry

        lax.fori_loop(0, take // chunk, narrow, 0)

    norm_shape = (jax.ShapeDtypeStruct((1, genes), jnp.float32),) if with_norm else ()
    norm_spec = [pl.BlockSpec((1, genes), lambda i, m, r: (0, 0))] if with_norm else []
    return pl.pallas_call(
        kernel,
        out_shape=(jax.ShapeDtypeStruct((share, genes), jnp.bfloat16), *norm_shape),
        grid_spec=pltpu.PrefetchScalarGridSpec(
            num_scalar_prefetch=2,
            grid=(share // take,),
            in_specs=[pl.BlockSpec((rows, genes), lambda i, m, r: (0, 0), pipeline_mode=pl.Buffered(1))],
            out_specs=[pl.BlockSpec((take, genes), lambda i, m, r: (i, 0)), *norm_spec],
            scratch_shapes=[
                pltpu.VMEM((rows * parts, LANES), jnp.float32),
                pltpu.VMEM((take * parts, LANES), jnp.float32),
            ],
        ),
        cost_estimate=pl.CostEstimate(flops=8 * 10**9, bytes_accessed=4 * rows * genes, transcendentals=0),
        compiler_params=pltpu.CompilerParams(vmem_limit_bytes=34 * 2**20),
        name="match",
    )(block_map, expr_row, expression)


def split_terms(value):
    high = value.astype(jnp.bfloat16)
    rest = value - high.astype(jnp.float32)
    middle = rest.astype(jnp.bfloat16)
    low = (rest - middle.astype(jnp.float32)).astype(jnp.bfloat16)
    return high, middle, low


def spread_left(value, axis):
    high, middle, low = split_terms(value)
    return jnp.concatenate([high, high, middle, high, middle, low], axis=axis)


def spread_right(value, axis):
    high, middle, low = split_terms(value)
    return jnp.concatenate([high, middle, high, low, middle, high], axis=axis)


def slot_specs(matched, slots, rows, genes):
    half = matched[0].shape[0] // rows
    arrays = [matched[slot // half] for slot in slots]
    return arrays, [pl.BlockSpec((rows, genes), lambda i, slot=slot: (slot % half, 0)) for slot in slots]


def square_lanes(value):
    wide = value.astype(jnp.float32)
    wide = wide * wide
    total = wide[:, :LANES]
    for part in range(1, wide.shape[1] // LANES):
        total = total + wide[:, part * LANES : (part + 1) * LANES]
    return total


def dot(x, y):
    return jnp.dot(x, y, preferred_element_type=jnp.float32)


def cov_spec(cov):
    array, start, rows = cov
    samples = array.shape[1]
    return pl.BlockSpec((pl.Element(rows), pl.Element(samples)), lambda i: (start, 0))


def piece_spec(piece, tile, at=lambda i: i):
    array, start = piece
    return pl.BlockSpec((pl.Element(tile), pl.Element(array.shape[1])), lambda i: (pl.multiple_of(start + at(i) * tile, 16), 0))


def over(x, y):
    return lax.dot_general(x, y, (((1,), (1,)), ((), ())), preferred_element_type=jnp.float32)


def fold_in(pieces, covars, matched, slots, width, state, grams):
    count = len(pieces)
    samples = pieces[0][0].shape[1]
    genes = matched[0].shape[1]
    covs = covars[0][2]
    tile = 256
    first = state is None
    with_grams = grams is not False
    rows = count * samples // len(slots)
    olds = (() if first else tuple(state)) + (tuple(grams) if with_grams and grams is not None else ())

    def kernel(*refs):
        piece_refs = refs[:count]
        covar_refs = refs[count : 2 * count]
        matched_refs = refs[2 * count : 2 * count + len(slots)]
        rest = refs[2 * count + len(slots) :]
        old_refs = rest[: len(olds)]
        outs = rest[len(olds) :]
        whole = jnp.concatenate([ref[...] for ref in piece_refs], axis=1)
        cov = jnp.concatenate([ref[...] for ref in covar_refs], axis=1)
        mine = jnp.concatenate([ref[...] for ref in matched_refs], axis=0)
        sums = dot(whole, mine)
        loads = over(whole, cov)
        norms = square_lanes(whole)
        if not first:
            sums = sums + old_refs[0][...]
            loads = loads + old_refs[1][...]
            norms = norms + old_refs[2][...]
        outs[0][...] = sums
        outs[1][...] = loads
        outs[2][...] = norms
        if with_grams:

            @pl.when(pl.program_id(0) == 0)
            def _():
                gram = over(cov, cov)
                cross = dot(cov, mine)
                if grams is not None:
                    gram = gram + old_refs[-2][...]
                    cross = cross + old_refs[-1][...]
                outs[3][...] = gram
                outs[4][...] = cross

    matched_arrays, matched_specs = slot_specs(matched, slots, rows, genes)
    state_specs = [
        pl.BlockSpec((tile, genes), lambda i: (i, 0)),
        pl.BlockSpec((tile, covs), lambda i: (i, 0)),
        pl.BlockSpec((tile, LANES), lambda i: (i, 0)),
    ]
    gram_specs = [pl.BlockSpec((covs, covs), lambda i: (0, 0)), pl.BlockSpec((covs, genes), lambda i: (0, 0))]
    shapes = [
        jax.ShapeDtypeStruct((width, genes), jnp.float32),
        jax.ShapeDtypeStruct((width, covs), jnp.float32),
        jax.ShapeDtypeStruct((width, LANES), jnp.float32),
    ]
    if with_grams:
        shapes += [jax.ShapeDtypeStruct((covs, covs), jnp.float32), jax.ShapeDtypeStruct((covs, genes), jnp.float32)]
    operands = [*[piece[0] for piece in pieces], *[cov[0] for cov in covars], *matched_arrays, *olds]
    results = pl.pallas_call(
        kernel,
        out_shape=tuple(shapes),
        grid=(width // tile,),
        in_specs=[piece_spec(piece, tile) for piece in pieces]
        + [cov_spec(cov) for cov in covars]
        + matched_specs
        + ([] if first else state_specs)
        + (gram_specs if with_grams and grams is not None else []),
        out_specs=tuple(state_specs + (gram_specs if with_grams else [])),
        input_output_aliases={} if first else {2 * count + len(slots) + k: k for k in range(3)},
        cost_estimate=pl.CostEstimate(
            flops=2 * width * samples * count * (genes + covs), bytes_accessed=8 * width * genes, transcendentals=0
        ),
        compiler_params=pltpu.CompilerParams(vmem_limit_bytes=24 * 2**20),
        name="fold",
    )(*operands)
    return results[:3], results[3:]


def whiten(covars, matched, slots, grams):
    count = len(covars)
    samples = covars[0][0].shape[1]
    genes = matched[0].shape[1]
    covs = covars[0][2]
    rows = count * samples // len(slots)
    matched_arrays, matched_specs = slot_specs(matched, slots, rows, genes)

    def kernel(*refs):
        covar_refs = refs[:count]
        matched_refs = refs[count : count + len(slots)]
        gram_ref, cross_ref, inverse_ref, loading_ref = refs[count + len(slots) :]
        cov = jnp.concatenate([ref[...] for ref in covar_refs], axis=1)
        mine = jnp.concatenate([ref[...] for ref in matched_refs], axis=0)
        cross = cross_ref[...] + dot(cov, mine)
        gram = gram_ref[...] + over(cov, cov)
        pad = jnp.zeros((covs, LANES - covs), jnp.float32)
        row_at = lax.broadcasted_iota(jnp.int32, (covs, LANES), 0)
        lane_at = lax.broadcasted_iota(jnp.int32, (covs, LANES), 1)
        at = lax.broadcasted_iota(jnp.int32, (covs, 1), 0)
        group = 8

        def eliminate(turn, pair):
            live, grown = pair
            undone = at < covs - turn * group
            for j in range(group):
                factor = jnp.where((at > j) & undone, live[:, j : j + 1] * (1.0 / live[j : j + 1, j : j + 1]), 0.0)
                live = live - factor * live[j : j + 1, :]
                grown = grown - factor * grown[j : j + 1, :]
            diagonal = jnp.sum(
                jnp.where(row_at[:group, :] == lane_at[:group, :], live[:group, :], 0.0), axis=1, keepdims=True
            )
            done = grown[:group, :] * lax.rsqrt(diagonal)
            inverse_ref[pl.ds(pl.multiple_of(turn * group, group), group), :] = done[:, :covs]
            live = pltpu.roll(jnp.concatenate([live[group:, :], live[:group, :]], axis=0), LANES - group, 1)
            grown = jnp.concatenate([grown[group:, :], grown[:group, :]], axis=0)
            return live, grown

        pair = (jnp.concatenate([gram, pad], axis=1), jnp.where(row_at == lane_at, 1.0, 0.0))
        lax.fori_loop(0, covs // group, eliminate, pair)
        loading_ref[...] = jnp.dot(inverse_ref[...], cross, precision=lax.Precision.HIGHEST)

    return pl.pallas_call(
        kernel,
        out_shape=(jax.ShapeDtypeStruct((covs, covs), jnp.float32), jax.ShapeDtypeStruct((covs, genes), jnp.float32)),
        grid=(1,),
        in_specs=[cov_spec(cov) for cov in covars]
        + matched_specs
        + [pl.BlockSpec((covs, covs), lambda i: (0, 0)), pl.BlockSpec((covs, genes), lambda i: (0, 0))],
        out_specs=(pl.BlockSpec((covs, covs), lambda i: (0, 0)), pl.BlockSpec((covs, genes), lambda i: (0, 0))),
        cost_estimate=pl.CostEstimate(flops=8 * 10**9, bytes_accessed=2 * rows * genes, transcendentals=0),
        compiler_params=pltpu.CompilerParams(vmem_limit_bytes=16 * 2**20),
        name="whiten",
    )(*[cov[0] for cov in covars], *matched_arrays, *grams)


def finish(full, low, high, covars, matched, slots, state, inverse, loading, panel_norm, scale, out, half, halves):
    count = len(low)
    more = len(full)
    samples = low[0][0].shape[1]
    genes = matched[0].shape[1]
    covs = covars[0][2]
    width = state[0].shape[0]
    tile = 512
    steps = width // tile
    split = steps // 2
    rows = (count + more) * samples // len(slots)
    matched_arrays, matched_specs = slot_specs(matched, slots, rows, genes)

    def kernel(*refs):
        refs = list(refs)

        def take(number):
            taken = refs[:number]
            del refs[:number]
            return taken

        full_refs, low_refs, high_refs, covar_refs = take(more), take(count), take(count), take(more + count)
        matched_refs = take(len(slots))
        sum_ref, load_ref, square_ref, inverse_ref, loading_ref, panel_ref = take(6)
        out_ref = refs[-1]
        here = pl.program_id(0)
        lasts = [jnp.where(here < split, one[...], other[...]) for one, other in zip(low_refs, high_refs)]
        whole = jnp.concatenate([ref[...] for ref in full_refs] + lasts, axis=1)
        cov = jnp.concatenate([ref[...] for ref in covar_refs], axis=1)
        mine = jnp.concatenate([ref[...] for ref in matched_refs], axis=0)
        sums = sum_ref[...] + dot(whole, mine)
        loads = load_ref[...] + over(whole, cov)
        squares = jnp.sum(square_ref[...] + square_lanes(whole), axis=1, keepdims=True)
        white = over(spread_left(loads, 1), spread_right(inverse_ref[...], 1))
        fitted = dot(spread_left(white, 1), spread_right(loading_ref[...], 0))
        resid_norm = jnp.maximum(squares - jnp.sum(white * white, axis=1, keepdims=True), 0.0)
        gain = scale * lax.rsqrt(resid_norm + epsilon)
        out_ref[...] = (sums - fitted) * gain * lax.rsqrt(panel_ref[...] + epsilon)

    operands = [*[piece[0] for piece in (*full, *low, *high)], *[cov[0] for cov in covars], *matched_arrays]
    operands += [*state, inverse, loading, panel_norm]
    in_specs = (
        [piece_spec(piece, tile) for piece in full]
        + [piece_spec(piece, tile, lambda i: jnp.minimum(i, split - 1)) for piece in low]
        + [piece_spec(piece, tile, lambda i: jnp.maximum(i - split, 0)) for piece in high]
        + [cov_spec(cov) for cov in covars]
        + matched_specs
        + [
            pl.BlockSpec((tile, genes), lambda i: (i, 0)),
            pl.BlockSpec((tile, covs), lambda i: (i, 0)),
            pl.BlockSpec((tile, LANES), lambda i: (i, 0)),
            pl.BlockSpec((covs, covs), lambda i: (0, 0)),
            pl.BlockSpec((covs, genes), lambda i: (0, 0)),
            pl.BlockSpec((1, genes), lambda i: (0, 0)),
        ]
    )
    aliases = {}
    if out is not None:
        aliases = {len(operands): 0}
        operands.append(out)
        in_specs.append(pl.BlockSpec(memory_space=pl.ANY))
    return pl.pallas_call(
        kernel,
        out_shape=jax.ShapeDtypeStruct((halves * width, genes), jnp.float32),
        grid=(steps,),
        in_specs=in_specs,
        out_specs=pl.BlockSpec((tile, genes), lambda i: (half * steps + i, 0)),
        input_output_aliases=aliases,
        cost_estimate=pl.CostEstimate(
            flops=2 * width * samples * (count + more) * genes + 14 * width * covs * genes,
            bytes_accessed=8 * width * genes,
            transcendentals=0,
        ),
        compiler_params=pltpu.CompilerParams(vmem_limit_bytes=20 * 2**20),
        name="finish",
    )(*operands)


def whole(dosage, covariates, expression, block_index, expr_row):
    blocks = block_index.shape[0]
    covars = covariates.shape[1]
    here = dosage.shape[0]
    ring = lax.axis_size("samp_0")
    turns = ring // 2
    chip = lax.axis_index("samp_0")
    core = lax.axis_index("samp_1")
    scale = math.sqrt(expr_row.shape[0] - covars - 1)
    up = [(i, (i + 1) % ring) for i in range(ring)]
    down = [(i, (i - 1) % ring) for i in range(ring)]
    cross = [(0, 1), (1, 0)]

    def swap(x):
        return lax.ppermute(x, "samp_1", cross)

    order = [chip]
    for turn in range(1, turns):
        order += [chip - turn, chip + turn]
    order += [chip + turns]
    order = [chip_at % ring for chip_at in order]
    block_map = jnp.stack([2 * chip_at + side for chip_at in order for side in (core, 1 - core)]).astype(jnp.int32)

    def trade(arrays):
        joined, starts = join(arrays)
        swapped = swap(joined)
        return [(swapped, start) for start in starts]

    def shift(values, turn):
        up_value, down_value = values
        if turn == turns:
            middle = width // 2
            up_value, down_value = up_value[:middle], down_value[middle:width]
        up_value = lax.ppermute(up_value, "samp_0", up)
        down_value = lax.ppermute(down_value, "samp_0", down)
        return up_value, down_value

    width = block_index.shape[1]
    own_cov = covariates.T
    next_cov = shift((own_cov, own_cov), 0)
    flow = [None] * blocks
    arrived = [{} for _ in range(blocks)]
    for block in range(blocks):
        if block == 0:
            pieces = pick_columns(dosage, block_index, block, covars, 2)
        else:
            pieces = pick_columns(dosage, block_index, block, 0, 1)
        if block == 0:
            pieces = ride(pieces, next_cov, width)
        flow[block] = (pieces[0], pieces[-1])
    own = [flow[block][0] for block in range(blocks)]
    covs = {}
    middle = block_map.shape[0] // 2
    first_rows, panel_norm = match_rows(expression, expr_row, block_map, here, 0, middle, True)
    (last_rows,) = match_rows(expression, expr_row, block_map, here, middle, middle, False)
    matched = (first_rows, last_rows)

    def inputs(turns_here, block):
        slots = []
        pieces = []
        covars_here = []
        for turn in turns_here:
            slots += [0] if turn == 0 else [2 * turn - 1, 2 * turn]
            pieces += arrived[block][turn]
            covars_here += covs[turn]
        return tuple(pieces), tuple(covars_here), matched, tuple(slots), width

    state = [None] * blocks
    grams = None

    def arrive(block, turn, pieces):
        arrived[block][turn] = pieces
        if block == 0:
            riders = tuple((array, start + width, covars) for array, start in pieces)
            covs[turn + 1] = riders if turn + 1 < turns else riders[:2]

    for turn in range(1, turns):
        for block in range(blocks):
            flow[block] = shift(flow[block], turn)
            if turn == turns - 1:
                up_swap, down_swap = trade(flow[block])
                arrive(block, turn, ((flow[block][0], 0), up_swap, (flow[block][1], 0), down_swap))
        if turn < turns - 1:
            arrays = [array for block in range(blocks) for array in flow[block]]
            if turn == 1:
                arrays += [*own, own_cov, *next_cov]
            traded = trade(arrays)
            for block in range(blocks):
                (up_value, down_value), (up_swap, down_swap) = flow[block], traded[2 * block : 2 * block + 2]
                arrive(block, turn, ((up_value, 0), up_swap, (down_value, 0), down_swap))
                if turn == 1:
                    arrived[block][0] = ((own[block], 0), traded[2 * blocks + block])
            if turn == 1:
                swapped_covs = [(*piece, covars) for piece in traded[3 * blocks :]]
                near = [((array, 0, covars), other) for array, other in zip((own_cov, *next_cov), swapped_covs)]
                covs[0] = near[0]
                covs[1] = (*near[1], *near[2])
        if turn % 2 == 0:
            ready = (0, 1, 2) if turn == 2 else (turn - 1, turn)
            for block in range(blocks):
                state[block], summed = fold_in(
                    *inputs(ready, block), state[block], grams if block == 0 else False
                )
                if block == 0:
                    grams = summed

    rest = (*covs[turns - 1], *covs[turns])
    last_slots = tuple(range(2 * turns - 3, 2 * turns))
    inverse, loading = whiten(rest, matched, last_slots, grams)

    out = None
    for block in range(blocks):
        flow[block] = shift(flow[block], turns)
        (low, high), (low_swap, high_swap) = flow[block], trade(flow[block])
        out = finish(
            arrived[block][turns - 1],
            ((low, 0), low_swap),
            ((high, 0), high_swap),
            rest,
            matched,
            last_slots,
            state[block],
            inverse,
            loading,
            panel_norm,
            scale,
            out,
            block,
            blocks,
        )
    return out


def solution(mesh):
    torus = Mesh(mesh.devices.reshape(mesh.shape["groups"], -1, 2), ("groups", "samp_0", "samp_1"))
    in_specs = (
        P(GROUPS_SAMP, None),
        P(GROUPS_SAMP, None),
        P("groups", SAMP),
        P("groups", None),
        P("groups"),
    )
    out_specs = P("groups", SAMP)
    return jax.shard_map(whole, mesh=torus, in_specs=in_specs, out_specs=out_specs, check_vma=False)
```

```python
import math

import jax
import jax.numpy as jnp
from jax import lax
from jax.experimental import pallas as pl
from jax.experimental.pallas import tpu as pltpu
from jax.sharding import Mesh
from jax.sharding import PartitionSpec as P


GROUPS_SAMP = ("groups", "samp_0", "samp_1")
SAMP = ("samp_0", "samp_1")
LANES = 128

epsilon = 1e-06


def pick_columns(dosage, block_index, block, extra, copies):
    samples, panel = dosage.shape
    blocks, width = block_index.shape
    span = 2048
    tile = 512
    spans = panel // span
    tiles = width // tile

    def kernel(index_ref, dosage_ref, *refs):
        index_at_ref, even_ref, odd_ref, sum_ref = refs[copies:]
        lane = lax.broadcasted_iota(jnp.int32, (LANES, LANES), 1)
        for part in range(width // LANES):
            row = index_ref[block : block + 1, part * LANES : (part + 1) * LANES].astype(jnp.float32)
            index_at_ref[part * LANES : (part + 1) * LANES, :] = (
                jnp.broadcast_to(row, (LANES, LANES)).T.astype(jnp.int32) - lane
            )

        def build(item, hot_ref):
            rows = pl.ds(pl.multiple_of((item // spans) * tile, tile), tile)
            column = index_at_ref[rows, :] - (item % spans) * span
            for step in range(span // LANES):
                hot_ref[:, step * LANES : (step + 1) * LANES] = jnp.where(column == step * LANES, 1.0, 0.0).astype(
                    jnp.bfloat16
                )

        def add(item, hot_ref):
            rows = pl.ds(pl.multiple_of((item // spans) * tile, tile), tile)
            span_at = item % spans
            columns = pl.ds(pl.multiple_of(span_at * span, span), span)
            picked = over(hot_ref[...], dosage_ref[:, columns])
            sum_ref[rows, :] = jnp.where(span_at == 0, 0.0, sum_ref[rows, :]) + picked

        def step(pair, carry):
            item = 2 * pair

            add(item, even_ref)
            build(item + 1, odd_ref)
            add(item + 1, odd_ref)
            build(jnp.minimum(item + 2, tiles * spans - 1), even_ref)
            return carry

        build(0, even_ref)
        lax.fori_loop(0, tiles * spans // 2, step, 0)
        for out_ref in refs[:copies]:
            out_ref[:width, :] = sum_ref[...].astype(jnp.bfloat16)

    return pl.pallas_call(
        kernel,
        out_shape=(jax.ShapeDtypeStruct((width + extra, samples), jnp.bfloat16),) * copies,
        grid=(1,),
        in_specs=[pl.BlockSpec((blocks, width), lambda i: (0, 0)), pl.BlockSpec((samples, panel), lambda i: (0, 0))],
        out_specs=(pl.BlockSpec((width + extra, samples), lambda i: (0, 0)),) * copies,
        scratch_shapes=[
            pltpu.VMEM((width, LANES), jnp.int32),
            pltpu.VMEM((tile, span), jnp.bfloat16),
            pltpu.VMEM((tile, span), jnp.bfloat16),
            pltpu.VMEM((width, samples), jnp.float32),
        ],
        cost_estimate=pl.CostEstimate(flops=2 * width * samples * panel, bytes_accessed=2 * samples * panel, transcendentals=0),
        compiler_params=pltpu.CompilerParams(vmem_limit_bytes=18 * 2**20),
        name="pick",
    )(block_index, dosage)


def ride(arrays, riders, width):
    count = len(arrays)
    rows, samples = riders[0].shape

    def kernel(*refs):
        for rider_ref, out_ref in zip(refs[count : 2 * count], refs[2 * count :]):
            out_ref[...] = rider_ref[...]

    block = pl.BlockSpec((pl.Element(rows), pl.Element(samples)), lambda i: (width, 0))
    return pl.pallas_call(
        kernel,
        out_shape=tuple(jax.ShapeDtypeStruct(array.shape, array.dtype) for array in arrays),
        grid=(1,),
        in_specs=[pl.BlockSpec(memory_space=pl.ANY)] * count + [pl.BlockSpec((rows, samples), lambda i: (0, 0))] * count,
        out_specs=(block,) * count,
        input_output_aliases={k: k for k in range(count)},
        cost_estimate=pl.CostEstimate(flops=6 * 10**9, bytes_accessed=4 * count * rows * samples, transcendentals=0),
        compiler_params=pltpu.CompilerParams(vmem_limit_bytes=8 * 2**20),
        name="ride",
    )(*arrays, *riders)


def join(arrays):
    samples = arrays[0].shape[1]
    starts = [0]
    for array in arrays:
        starts.append(starts[-1] + array.shape[0])

    def kernel(*refs):
        for ref, start in zip(refs[:-1], starts):
            refs[-1][start : start + ref.shape[0], :] = ref[...]

    joined = pl.pallas_call(
        kernel,
        out_shape=jax.ShapeDtypeStruct((starts[-1], samples), arrays[0].dtype),
        grid=(1,),
        in_specs=[pl.BlockSpec(array.shape, lambda i: (0, 0)) for array in arrays],
        out_specs=pl.BlockSpec((starts[-1], samples), lambda i: (0, 0)),
        compiler_params=pltpu.CompilerParams(vmem_limit_bytes=12 * 2**20),
        name="join",
    )(*arrays)
    return joined, starts[:-1]


def match_rows(expression, expr_row, block_map, block, first, count, with_norm):
    rows, genes = expression.shape
    parts = genes // LANES
    chunk = 128
    take = 4 * block

    share = count * block

    def kernel(map_ref, row_ref, exp_ref, out_ref, *refs):
        wide_ref, got_ref = refs[-2:]
        here = pl.program_id(0)

        @pl.when(here == 0)
        def _():
            def widen(step, sums):
                at = pl.multiple_of(step * chunk, chunk)
                value = exp_ref[pl.ds(at, chunk), :].astype(jnp.float32)
                for part in range(parts):
                    wide_ref[pl.ds(at * parts + part, chunk, stride=parts), :] = value[:, part * LANES : (part + 1) * LANES]
                if not with_norm:
                    return sums
                square = value * value
                return sums + jnp.sum(square.reshape(chunk // 8, 8, genes), axis=0)

            sums = lax.fori_loop(0, rows // chunk, widen, jnp.zeros((8, genes), jnp.float32))
            if with_norm:
                refs[0][...] = jnp.sum(sums, axis=0, keepdims=True)

        unroll = 64

        def fetch(step, carry):
            at = step * unroll
            base = map_ref[first + here * (take // block) + at // block] * block - (at // block) * block
            for k in range(unroll):
                source = pl.multiple_of(row_ref[base + at + k] * parts, parts)
                target = pl.multiple_of((at + k) * parts, parts)
                got_ref[pl.ds(target, parts), :] = wide_ref[pl.ds(source, parts), :]
            return carry

        lax.fori_loop(0, take // unroll, fetch, 0)

        def narrow(step, carry):
            at = pl.multiple_of(step * chunk, chunk)
            for part in range(parts):
                value = got_ref[pl.ds(at * parts + part, chunk, stride=parts), :]
                out_ref[pl.ds(at, chunk), part * LANES : (part + 1) * LANES] = value.astype(jnp.bfloat16)
            return carry

        lax.fori_loop(0, take // chunk, narrow, 0)

    norm_shape = (jax.ShapeDtypeStruct((1, genes), jnp.float32),) if with_norm else ()
    norm_spec = [pl.BlockSpec((1, genes), lambda i, m, r: (0, 0))] if with_norm else []
    return pl.pallas_call(
        kernel,
        out_shape=(jax.ShapeDtypeStruct((share, genes), jnp.bfloat16), *norm_shape),
        grid_spec=pltpu.PrefetchScalarGridSpec(
            num_scalar_prefetch=2,
            grid=(share // take,),
            in_specs=[pl.BlockSpec((rows, genes), lambda i, m, r: (0, 0), pipeline_mode=pl.Buffered(1))],
            out_specs=[pl.BlockSpec((take, genes), lambda i, m, r: (i, 0)), *norm_spec],
            scratch_shapes=[
                pltpu.VMEM((rows * parts, LANES), jnp.float32),
                pltpu.VMEM((take * parts, LANES), jnp.float32),
            ],
        ),
        cost_estimate=pl.CostEstimate(flops=8 * 10**9, bytes_accessed=4 * rows * genes, transcendentals=0),
        compiler_params=pltpu.CompilerParams(vmem_limit_bytes=31 * 2**20),
        name="match",
    )(block_map, expr_row, expression)


def split_terms(value):
    high = value.astype(jnp.bfloat16)
    rest = value - high.astype(jnp.float32)
    middle = rest.astype(jnp.bfloat16)
    low = (rest - middle.astype(jnp.float32)).astype(jnp.bfloat16)
    return high, middle, low


def spread_left(value, axis):
    high, middle, low = split_terms(value)
    return jnp.concatenate([high, high, middle, high, middle, low], axis=axis)


def spread_right(value, axis):
    high, middle, low = split_terms(value)
    return jnp.concatenate([high, middle, high, low, middle, high], axis=axis)


def slot_specs(matched, slots, rows, genes):
    places = [(array, block) for array in matched for block in range(array.shape[0] // rows)]
    arrays = [places[slot][0] for slot in slots]
    return arrays, [pl.BlockSpec((rows, genes), lambda i, at=places[slot][1]: (at, 0)) for slot in slots]


def square_lanes(value):
    wide = value.astype(jnp.float32)
    wide = wide * wide
    total = wide[:, :LANES]
    for part in range(1, wide.shape[1] // LANES):
        total = total + wide[:, part * LANES : (part + 1) * LANES]
    return total


def dot(x, y):
    return jnp.dot(x, y, preferred_element_type=jnp.float32)


def cov_spec(cov):
    array, start, rows = cov
    samples = array.shape[1]
    return pl.BlockSpec((pl.Element(rows), pl.Element(samples)), lambda i: (start, 0))


def piece_spec(piece, tile, at=lambda i: i):
    array, start = piece
    return pl.BlockSpec((pl.Element(tile), pl.Element(array.shape[1])), lambda i: (pl.multiple_of(start + at(i) * tile, 16), 0))


def over(x, y):
    return lax.dot_general(x, y, (((1,), (1,)), ((), ())), preferred_element_type=jnp.float32)


def fold_in(pieces, covars, matched, slots, width, state, grams):
    count = len(pieces)
    samples = pieces[0][0].shape[1]
    genes = matched[0].shape[1]
    covs = covars[0][2]
    tile = 256
    first = state is None
    with_grams = grams is not False
    rows = count * samples // len(slots)
    olds = (() if first else tuple(state)) + (tuple(grams) if with_grams and grams is not None else ())

    def kernel(*refs):
        piece_refs = refs[:count]
        covar_refs = refs[count : 2 * count]
        matched_refs = refs[2 * count : 2 * count + len(slots)]
        rest = refs[2 * count + len(slots) :]
        old_refs = rest[: len(olds)]
        outs = rest[len(olds) :]
        whole = jnp.concatenate([ref[...] for ref in piece_refs], axis=1)
        cov = jnp.concatenate([ref[...] for ref in covar_refs], axis=1)
        mine = jnp.concatenate([ref[...] for ref in matched_refs], axis=0)
        sums = dot(whole, mine)
        loads = over(whole, cov)
        norms = square_lanes(whole)
        if not first:
            sums = sums + old_refs[0][...]
            loads = loads + old_refs[1][...]
            norms = norms + old_refs[2][...]
        outs[0][...] = sums
        outs[1][...] = loads
        outs[2][...] = norms
        if with_grams:

            @pl.when(pl.program_id(0) == 0)
            def _():
                gram = over(cov, cov)
                cross = dot(cov, mine)
                if grams is not None:
                    gram = gram + old_refs[-2][...]
                    cross = cross + old_refs[-1][...]
                outs[3][...] = gram
                outs[4][...] = cross

    matched_arrays, matched_specs = slot_specs(matched, slots, rows, genes)
    state_specs = [
        pl.BlockSpec((tile, genes), lambda i: (i, 0)),
        pl.BlockSpec((tile, covs), lambda i: (i, 0)),
        pl.BlockSpec((tile, LANES), lambda i: (i, 0)),
    ]
    gram_specs = [pl.BlockSpec((covs, covs), lambda i: (0, 0)), pl.BlockSpec((covs, genes), lambda i: (0, 0))]
    shapes = [
        jax.ShapeDtypeStruct((width, genes), jnp.float32),
        jax.ShapeDtypeStruct((width, covs), jnp.float32),
        jax.ShapeDtypeStruct((width, LANES), jnp.float32),
    ]
    if with_grams:
        shapes += [jax.ShapeDtypeStruct((covs, covs), jnp.float32), jax.ShapeDtypeStruct((covs, genes), jnp.float32)]
    operands = [*[piece[0] for piece in pieces], *[cov[0] for cov in covars], *matched_arrays, *olds]
    results = pl.pallas_call(
        kernel,
        out_shape=tuple(shapes),
        grid=(width // tile,),
        in_specs=[piece_spec(piece, tile) for piece in pieces]
        + [cov_spec(cov) for cov in covars]
        + matched_specs
        + ([] if first else state_specs)
        + (gram_specs if with_grams and grams is not None else []),
        out_specs=tuple(state_specs + (gram_specs if with_grams else [])),
        input_output_aliases={} if first else {2 * count + len(slots) + k: k for k in range(3)},
        cost_estimate=pl.CostEstimate(
            flops=2 * width * samples * count * (genes + covs), bytes_accessed=8 * width * genes, transcendentals=0
        ),
        compiler_params=pltpu.CompilerParams(vmem_limit_bytes=18 * 2**20),
        name="fold",
    )(*operands)
    return results[:3], results[3:]


def whiten(covars, matched, slots, grams):
    count = len(covars)
    samples = covars[0][0].shape[1]
    genes = matched[0].shape[1]
    covs = covars[0][2]
    rows = count * samples // len(slots)
    matched_arrays, matched_specs = slot_specs(matched, slots, rows, genes)

    def kernel(*refs):
        covar_refs = refs[:count]
        matched_refs = refs[count : count + len(slots)]
        gram_ref, cross_ref, inverse_ref, loading_ref = refs[count + len(slots) :]
        cov = jnp.concatenate([ref[...] for ref in covar_refs], axis=1)
        mine = jnp.concatenate([ref[...] for ref in matched_refs], axis=0)
        cross = cross_ref[...] + dot(cov, mine)
        gram = gram_ref[...] + over(cov, cov)
        pad = jnp.zeros((covs, LANES - covs), jnp.float32)
        row_at = lax.broadcasted_iota(jnp.int32, (covs, LANES), 0)
        lane_at = lax.broadcasted_iota(jnp.int32, (covs, LANES), 1)
        at = lax.broadcasted_iota(jnp.int32, (covs, 1), 0)
        group = 24

        def eliminate(turn, pair):
            live, grown = pair
            undone = at < covs - turn * group
            for j in range(group):
                factor = jnp.where((at > j) & undone, live[:, j : j + 1] * (1.0 / live[j : j + 1, j : j + 1]), 0.0)
                live = live - factor * live[j : j + 1, :]
                grown = grown - factor * grown[j : j + 1, :]
            diagonal = jnp.sum(
                jnp.where(row_at[:group, :] == lane_at[:group, :], live[:group, :], 0.0), axis=1, keepdims=True
            )
            done = grown[:group, :] * lax.rsqrt(diagonal)
            inverse_ref[pl.ds(pl.multiple_of(turn * group, group), group), :] = done[:, :covs]
            live = pltpu.roll(jnp.concatenate([live[group:, :], live[:group, :]], axis=0), LANES - group, 1)
            grown = jnp.concatenate([grown[group:, :], grown[:group, :]], axis=0)
            return live, grown

        pair = (jnp.concatenate([gram, pad], axis=1), jnp.where(row_at == lane_at, 1.0, 0.0))
        lax.fori_loop(0, covs // group, eliminate, pair)
        loading_ref[...] = jnp.dot(inverse_ref[...], cross, precision=lax.Precision.HIGHEST)

    return pl.pallas_call(
        kernel,
        out_shape=(jax.ShapeDtypeStruct((covs, covs), jnp.float32), jax.ShapeDtypeStruct((covs, genes), jnp.float32)),
        grid=(1,),
        in_specs=[cov_spec(cov) for cov in covars]
        + matched_specs
        + [pl.BlockSpec((covs, covs), lambda i: (0, 0)), pl.BlockSpec((covs, genes), lambda i: (0, 0))],
        out_specs=(pl.BlockSpec((covs, covs), lambda i: (0, 0)), pl.BlockSpec((covs, genes), lambda i: (0, 0))),
        cost_estimate=pl.CostEstimate(flops=8 * 10**9, bytes_accessed=2 * rows * genes, transcendentals=0),
        compiler_params=pltpu.CompilerParams(vmem_limit_bytes=16 * 2**20),
        name="whiten",
    )(*[cov[0] for cov in covars], *matched_arrays, *grams)


def finish(full, low, high, covars, matched, slots, state, inverse, loading, panel_norm, scale, out, half, halves):
    count = len(low)
    more = len(full)
    samples = low[0][0].shape[1]
    genes = matched[0].shape[1]
    covs = covars[0][2]
    width = state[0].shape[0]
    tile = 512
    steps = width // tile
    split = steps // 2
    rows = (count + more) * samples // len(slots)
    matched_arrays, matched_specs = slot_specs(matched, slots, rows, genes)

    def kernel(*refs):
        refs = list(refs)

        def take(number):
            taken = refs[:number]
            del refs[:number]
            return taken

        full_refs, low_refs, high_refs, covar_refs = take(more), take(count), take(count), take(more + count)
        matched_refs = take(len(slots))
        sum_ref, load_ref, square_ref, inverse_ref, loading_ref, panel_ref = take(6)
        out_ref = refs[-1]
        here = pl.program_id(0)
        lasts = [jnp.where(here < split, one[...], other[...]) for one, other in zip(low_refs, high_refs)]
        whole = jnp.concatenate([ref[...] for ref in full_refs] + lasts, axis=1)
        cov = jnp.concatenate([ref[...] for ref in covar_refs], axis=1)
        mine = jnp.concatenate([ref[...] for ref in matched_refs], axis=0)
        sums = sum_ref[...] + dot(whole, mine)
        loads = load_ref[...] + over(whole, cov)
        squares = jnp.sum(square_ref[...] + square_lanes(whole), axis=1, keepdims=True)
        white = over(spread_left(loads, 1), spread_right(inverse_ref[...], 1))
        fitted = dot(spread_left(white, 1), spread_right(loading_ref[...], 0))
        resid_norm = jnp.maximum(squares - jnp.sum(white * white, axis=1, keepdims=True), 0.0)
        gain = scale * lax.rsqrt(resid_norm + epsilon)
        out_ref[...] = (sums - fitted) * gain * lax.rsqrt(panel_ref[...] + epsilon)

    operands = [*[piece[0] for piece in (*full, *low, *high)], *[cov[0] for cov in covars], *matched_arrays]
    operands += [*state, inverse, loading, panel_norm]
    in_specs = (
        [piece_spec(piece, tile) for piece in full]
        + [piece_spec(piece, tile, lambda i: jnp.minimum(i, split - 1)) for piece in low]
        + [piece_spec(piece, tile, lambda i: jnp.maximum(i - split, 0)) for piece in high]
        + [cov_spec(cov) for cov in covars]
        + matched_specs
        + [
            pl.BlockSpec((tile, genes), lambda i: (i, 0)),
            pl.BlockSpec((tile, covs), lambda i: (i, 0)),
            pl.BlockSpec((tile, LANES), lambda i: (i, 0)),
            pl.BlockSpec((covs, covs), lambda i: (0, 0)),
            pl.BlockSpec((covs, genes), lambda i: (0, 0)),
            pl.BlockSpec((1, genes), lambda i: (0, 0)),
        ]
    )
    aliases = {}
    if out is not None:
        aliases = {len(operands): 0}
        operands.append(out)
        in_specs.append(pl.BlockSpec(memory_space=pl.ANY))
    return pl.pallas_call(
        kernel,
        out_shape=jax.ShapeDtypeStruct((halves * width, genes), jnp.float32),
        grid=(steps,),
        in_specs=in_specs,
        out_specs=pl.BlockSpec((tile, genes), lambda i: (half * steps + i, 0)),
        input_output_aliases=aliases,
        cost_estimate=pl.CostEstimate(
            flops=2 * width * samples * (count + more) * genes + 14 * width * covs * genes,
            bytes_accessed=8 * width * genes,
            transcendentals=0,
        ),
        compiler_params=pltpu.CompilerParams(vmem_limit_bytes=16 * 2**20),
        name="finish",
    )(*operands)


def whole(dosage, covariates, expression, block_index, expr_row):
    blocks = block_index.shape[0]
    covars = covariates.shape[1]
    here = dosage.shape[0]
    ring = lax.axis_size("samp_0")
    turns = ring // 2
    chip = lax.axis_index("samp_0")
    core = lax.axis_index("samp_1")
    scale = math.sqrt(expr_row.shape[0] - covars - 1)
    up = [(i, (i + 1) % ring) for i in range(ring)]
    down = [(i, (i - 1) % ring) for i in range(ring)]
    cross = [(0, 1), (1, 0)]

    def swap(x):
        return lax.ppermute(x, "samp_1", cross)

    order = [chip]
    for turn in range(1, turns):
        order += [chip - turn, chip + turn]
    order += [chip + turns]
    order = [chip_at % ring for chip_at in order]
    block_map = jnp.stack([2 * chip_at + side for chip_at in order for side in (core, 1 - core)]).astype(jnp.int32)

    def trade(arrays):
        joined, starts = join(arrays)
        swapped = swap(joined)
        return [(swapped, start) for start in starts]

    def shift(values, turn):
        up_value, down_value = values
        if turn == turns:
            middle = width // 2
            up_value, down_value = up_value[:middle], down_value[middle:width]
        up_value = lax.ppermute(up_value, "samp_0", up)
        down_value = lax.ppermute(down_value, "samp_0", down)
        return up_value, down_value

    width = block_index.shape[1]
    own_cov = covariates.T
    next_cov = shift((own_cov, own_cov), 0)
    flow = [None] * blocks
    arrived = [{} for _ in range(blocks)]
    for block in range(blocks):
        if block == 0:
            pieces = pick_columns(dosage, block_index, block, covars, 2)
        else:
            pieces = pick_columns(dosage, block_index, block, 0, 1)
        if block == 0:
            pieces = ride(pieces, next_cov, width)
        flow[block] = (pieces[0], pieces[-1])
    own = [flow[block][0] for block in range(blocks)]
    covs = {}
    shares = block_map.shape[0]
    matched = []
    for part, (begin, end) in enumerate(((0, shares // 4), (shares // 4, 5 * shares // 8), (5 * shares // 8, shares))):
        found, *norms = match_rows(expression, expr_row, block_map, here, begin, end - begin, part == 2)
        matched.append(found)
    (panel_norm,) = norms

    def inputs(turns_here, block):
        slots = []
        pieces = []
        covars_here = []
        for turn in turns_here:
            slots += [0] if turn == 0 else [2 * turn - 1, 2 * turn]
            pieces += arrived[block][turn]
            covars_here += covs[turn]
        return tuple(pieces), tuple(covars_here), matched, tuple(slots), width

    state = [None] * blocks
    grams = None
    folds = fold_turns(turns)

    def arrive(block, turn, pieces):
        arrived[block][turn] = pieces
        if block == 0:
            riders = tuple((array, start + width, covars) for array, start in pieces)
            covs[turn + 1] = riders if turn + 1 < turns else riders[:2]

    for turn in range(1, turns):
        for block in range(blocks):
            flow[block] = shift(flow[block], turn)
            if turn == turns - 1:
                up_swap, down_swap = trade(flow[block])
                arrive(block, turn, ((flow[block][0], 0), up_swap, (flow[block][1], 0), down_swap))
        if turn < turns - 1:
            arrays = [array for block in range(blocks) for array in flow[block]]
            if turn == 1:
                arrays += [*own, own_cov, *next_cov]
            traded = trade(arrays)
            for block in range(blocks):
                (up_value, down_value), (up_swap, down_swap) = flow[block], traded[2 * block : 2 * block + 2]
                arrive(block, turn, ((up_value, 0), up_swap, (down_value, 0), down_swap))
                if turn == 1:
                    arrived[block][0] = ((own[block], 0), traded[2 * blocks + block])
            if turn == 1:
                swapped_covs = [(*piece, covars) for piece in traded[3 * blocks :]]
                near = [((array, 0, covars), other) for array, other in zip((own_cov, *next_cov), swapped_covs)]
                covs[0] = near[0]
                covs[1] = (*near[1], *near[2])
        if turn in folds:
            ready = tuple(range(max([0] + [stop + 1 for stop in folds if stop < turn]), turn + 1))
            for block in range(blocks):
                state[block], summed = fold_in(
                    *inputs(ready, block), state[block], grams if block == 0 else False
                )
                if block == 0:
                    grams = summed

    rest = (*covs[turns - 1], *covs[turns])
    last_slots = tuple(range(2 * turns - 3, 2 * turns))
    inverse, loading = whiten(rest, matched, last_slots, grams)

    out = None
    for block in range(blocks):
        flow[block] = shift(flow[block], turns)
        (low, high), (low_swap, high_swap) = flow[block], trade(flow[block])
        out = finish(
            arrived[block][turns - 1],
            ((low, 0), low_swap),
            ((high, 0), high_swap),
            rest,
            matched,
            last_slots,
            state[block],
            inverse,
            loading,
            panel_norm,
            scale,
            out,
            block,
            blocks,
        )
    return out


def fold_turns(turns):
    return (2, turns - 3, turns - 2)


def solution(mesh):
    torus = Mesh(mesh.devices.reshape(mesh.shape["groups"], -1, 2), ("groups", "samp_0", "samp_1"))
    in_specs = (
        P(GROUPS_SAMP, None),
        P(GROUPS_SAMP, None),
        P("groups", SAMP),
        P("groups", None),
        P("groups"),
    )
    out_specs = P("groups", SAMP)
    return jax.shard_map(whole, mesh=torus, in_specs=in_specs, out_specs=out_specs, check_vma=False)
```
